256 devices in a mesh: cp: 64 (over z_hi, y, x, core), tp: 4 (over z_lo).
Axes of the slice: x: 4, y: 4, z: 8 (z_hi: 2, z_lo: 4; z = z_hi * 4 + z_lo), core: 2. Of those that a mesh axis runs over, the one named last changes fastest.
Arguments:
- queries: bfloat16 [49152, 5120], P('cp', 'tp'), may hold values from -36 to 36
- keys: bfloat16 [49152, 1024], P('cp', 'tp'), may hold values from -5 to 5
- values: bfloat16 [49152, 1024], P('cp', 'tp'), may hold values from -6 to 6
- doc_lengths: int32 [64], replicated, may hold values from 1 to 1536, 49152 in all
Outputs:
- attended: bfloat16 [49152, 5120], P(('cp', 'tp'))
The draws below stay inside these ranges and needn't reach their ends.
Inputs may be any that keep to these rules, and one draw needn't show every extreme that they name: `doc_lengths`: they sum to 49152, and one of them is exactly 1536.
All inputs are finite; a program needn't handle non-finite values.
Results may differ from the reference program's by a relative error of at most 0.0038.
Values may be sent and summed in bfloat16 or wider, within the bound.
A program may use at most 256 MiB of HBM per device.

```python
import math
import jax
import jax.numpy as jnp
import numpy as np
from jax import lax

Q_HEADS = 40
KV_HEADS = 8
HEAD = 128
TOK_DEV = 768
TOKENS = 49152
MAXDOC = 1536
NDOCS = 64
N_CP = 64


def draw_keys(key, part):
    drawn_draw = jnp.clip(jax.random.normal(jax.random.fold_in(key, 11), (TOKENS, KV_HEADS, HEAD), jnp.float32), -5.0, 5.0)
    result = drawn_draw
    return result.reshape(TOKENS, KV_HEADS * HEAD).astype(jnp.bfloat16)


def draw_queries(key, part):
    group_size = Q_HEADS // KV_HEADS
    drawn_draw = jnp.clip(jax.random.normal(jax.random.fold_in(key, 12), (TOKENS, KV_HEADS, group_size, HEAD), jnp.float32), -5.0, 5.0)
    result = drawn_draw
    return result.reshape(TOKENS, Q_HEADS * HEAD).astype(jnp.bfloat16)


def shard_levels(key, dims, split, low, largest):
    loudness, own = 1.0, jax.random.fold_in(key, 6)
    for dim, blocks in split:
        steps = jnp.exp(jax.random.uniform(jax.random.fold_in(own, dim), (blocks,), jnp.float32, low / len(split), largest / len(split)))
        loudness = loudness * jnp.repeat(steps, dims[dim] // blocks).reshape([-1 if axis == dim else 1 for axis in range(len(dims))])
    return loudness


def length_profile(number_of, total, most, slope):
    loads = [(1 << 20) // math.isqrt(standing ** slope) + 1 for standing in range(2, number_of + 1)]
    spare, counts = total - most - (number_of - 1), [1] * (number_of - 1)
    while spare > 0:
        candidates = [i for i in range(number_of - 1) if counts[i] < most]
        mass, left = sum([loads[i] for i in candidates]), spare
        for i in candidates:
            extra = min(most - counts[i], max(1, left * loads[i] // mass), spare)
            counts[i] = counts[i] + extra
            spare = spare - extra
    return np.array([most] + counts)


def ragged_sizes(own_key, amount, total, reach, skew):
    if amount == 2:
        one = jax.random.randint(own_key, (), max(1, total - reach), min(reach, total - 1) + 1)
        return jnp.stack([one, total - one])
    tallies = jnp.asarray(length_profile(amount, total, reach, skew), jnp.int32)
    twos = (amount - 1) // 2
    donor, receiver = tallies[1:1 + 2 * twos:2], tallies[2:2 + 2 * twos:2]
    margin = jnp.minimum(donor - 1, reach - receiver)
    passed = jax.random.randint(jax.random.fold_in(own_key, 1), (twos,), 0, 1 << 20) % (margin + 1)
    tallies = tallies.at[1:1 + 2 * twos:2].set(donor - passed).at[2:2 + 2 * twos:2].set(receiver + passed)
    return tallies[jax.random.permutation(jax.random.fold_in(own_key, 2), amount)]


def bell_draw(own_key, extent, width, most, split=(), held_as=jnp.bfloat16):
    values = jax.random.normal(own_key, extent, jnp.float32) * width
    if len(split) > 0:
        values = shard_levels(own_key, extent, split, -0.22, 0.18) * values
    return jnp.clip(values, min=-most, max=most).astype(held_as)


def setup_inputs(seed: int = 0) -> dict:
    splits = jax.random.split(jax.random.key(seed), 5)
    return {
        "queries": draw_queries(jax.random.fold_in(splits[4], 71), 0),
        "keys": draw_keys(jax.random.fold_in(splits[4], 71), 0),
        "values": bell_draw(splits[2], (TOKENS, KV_HEADS * HEAD), 1.0, 6.0, ((0, 64), (1, 4))),
        "doc_lengths": ragged_sizes(splits[3], NDOCS, TOKENS, MAXDOC, 2).astype(jnp.int32),
    }


negative = -1.0e30


def to_sequence(blocked):
    key_width = blocked.shape[1]
    parts = blocked.reshape(N_CP, 2, TOK_DEV // 2, key_width)
    return jnp.concatenate([parts[:, 0], parts[::-1, 1]], axis=0).reshape(TOKENS, key_width)


def reference(queries, keys, values, doc_lengths):
    half_rows = TOK_DEV // 2
    group_size = Q_HEADS // KV_HEADS
    seq_queries = to_sequence(queries).reshape(TOKENS, KV_HEADS, group_size, HEAD)
    seq_keys = to_sequence(keys).reshape(TOKENS, KV_HEADS, HEAD)
    seq_values = to_sequence(values).reshape(TOKENS, KV_HEADS, HEAD)
    doc_ends = jnp.cumsum(doc_lengths).astype(jnp.int32)
    positions = jnp.arange(TOKENS, dtype=jnp.int32)
    doc_ids = jnp.sum((positions[:, None] >= doc_ends[None, :]).astype(jnp.int32), axis=1).astype(jnp.int32)
    padded_keys = jnp.concatenate([jnp.zeros((MAXDOC, KV_HEADS, HEAD), seq_keys.dtype), seq_keys], axis=0)
    padded_values = jnp.concatenate([jnp.zeros((MAXDOC, KV_HEADS, HEAD), seq_values.dtype), seq_values], axis=0)
    padded_docs = jnp.concatenate([jnp.full((MAXDOC,), -1, jnp.int32), doc_ids], axis=0)
    key_width = MAXDOC + half_rows
    scale = float(HEAD) ** -0.5

    def one_block(block_index):
        row_start = (block_index * half_rows).astype(jnp.int32)
        query_block = lax.dynamic_slice_in_dim(seq_queries, row_start, half_rows, 0)
        key_block = lax.dynamic_slice_in_dim(padded_keys, row_start, key_width, 0)
        value_block = lax.dynamic_slice_in_dim(padded_values, row_start, key_width, 0)
        q_doc = lax.dynamic_slice_in_dim(doc_ids, row_start, half_rows, 0)
        k_doc = lax.dynamic_slice_in_dim(padded_docs, row_start, key_width, 0)
        q_pos = row_start + jnp.arange(half_rows, dtype=jnp.int32)
        k_pos = row_start - MAXDOC + jnp.arange(key_width, dtype=jnp.int32)
        allowed = (k_doc[None, :] == q_doc[:, None]) & (k_pos[None, :] <= q_pos[:, None])
        scores = jnp.einsum("qhjd,khd->qhjk", query_block.astype(jnp.float32), key_block.astype(jnp.float32)) * scale
        allowed_wide = allowed[:, None, None, :]
        masked = jnp.where(allowed_wide, scores, negative)
        row_max = jnp.max(masked, axis=-1, keepdims=True)
        weights = jnp.where(allowed_wide, jnp.exp(masked - row_max), 0.0)
        weight_sum = jnp.sum(weights, axis=-1)
        rounded = lax.optimization_barrier(weights.astype(jnp.bfloat16)).astype(jnp.float32)
        output = jnp.einsum("qhjk,khd->qhjd", rounded, value_block.astype(jnp.float32)) / weight_sum[..., None]
        return output.astype(jnp.bfloat16)

    blocks = lax.map(one_block, jnp.arange(2 * N_CP, dtype=jnp.int32))
    flattened = blocks.reshape(2 * N_CP, half_rows, Q_HEADS * HEAD)
    first_half = flattened[:N_CP]
    second_half = flattened[N_CP:][::-1]
    return jnp.stack([first_half, second_half], axis=1).reshape(TOKENS, Q_HEADS * HEAD)
```

```python
import functools
import math

import jax
import jax.numpy as jnp
from jax import lax
from jax.experimental import pallas as pl
from jax.experimental.pallas import tpu as pltpu
from jax.sharding import PartitionSpec as P

HEAD = 128
MESH = pl.DeviceIdType.MESH
MASKED = -1e30
KEY_TILE = 256


def other(bit):
    return 1 - bit


def kernel(sizes, lens_ref, q_hbm, k_hbm, v_hbm, out_hbm, kv, qbuf, bias, scores, outs,
           load_sem, q_sem, kv_send, kv_recv, out_send, out_recv, own_sem):
    cp_size, tp_size, half, groups, kv_local = sizes
    heads = groups * kv_local
    chunk = 2 * half // tp_size
    slots = 5
    window = bias.shape[-1]
    key_tiles = window // KEY_TILE
    cp = lax.axis_index("cp")
    tp = lax.axis_index("tp")
    core = cp % 2
    partner = cp + 1 - 2 * core

    def slot(direction, g, which):
        return kv.at[direction, g, :, pl.ds(which * half, half), :]

    at_end = [(cp >= cp_size - 2).astype(jnp.int32), (cp < 2).astype(jnp.int32)]
    beyond = [
        (1 - at_end[0]) * (cp + 2) + at_end[0] * partner,
        (1 - at_end[1]) * (cp - 2) + at_end[1] * partner,
    ]
    landing = [at_end[0], 1 - at_end[1]]
    is_lead = [core == 0, core == 1]
    lead_of = [1 - core, core]

    def load(direction, g, part):
        src = (k_hbm, v_hbm)[part]
        return pltpu.make_async_copy(
            src.at[pl.ds(direction * half, half), pl.ds(g * HEAD, HEAD)],
            kv.at[direction, g, part, pl.ds(4 * half, half), :],
            load_sem.at[direction, g, part],
        )

    def load_q(h):
        return pltpu.make_async_copy(
            q_hbm.at[:, pl.ds(h * HEAD, HEAD)], qbuf.at[h], q_sem.at[h]
        )

    def hop(direction, g, far):
        return pltpu.make_async_remote_copy(
            src_ref=slot(direction, g, 4 - 2 * far),
            dst_ref=slot(landing[direction], g, 2 - 2 * far),
            send_sem=kv_send.at[direction, g, far],
            recv_sem=kv_recv.at[landing[direction], g, 2 - 2 * far],
            device_id=(beyond[direction], tp),
            device_id_type=MESH,
        )

    def across(direction, g, far):
        lead = lead_of[direction]
        return pltpu.make_async_remote_copy(
            src_ref=slot(direction, g, 2 * lead + 2 - 2 * far),
            dst_ref=slot(direction, g, 3 - 2 * far),
            send_sem=kv_send.at[direction, g, 2 + far],
            recv_sem=kv_recv.at[direction, g, 3 - 2 * far],
            device_id=(partner, tp),
            device_id_type=MESH,
        )

    def arrived(direction, g, which):
        pltpu.make_async_remote_copy(
            src_ref=slot(direction, g, which),
            dst_ref=slot(direction, g, which),
            send_sem=kv_send.at[direction, g, 0],
            recv_sem=kv_recv.at[direction, g, which],
            device_id=(partner, tp),
            device_id_type=MESH,
        ).wait_recv()

    def peer_of(turn):
        n = 3 - turn
        high = (tp // 2 + n // 2) % 2
        low = (tp % 2 + n % 2 + n // 2) % 2
        return high, low

    def send(turn, h):
        high, low = peer_of(turn)
        return pltpu.make_async_remote_copy(
            src_ref=outs.at[turn, h],
            dst_ref=out_hbm.at[:, pl.ds((tp * heads + h) * HEAD, HEAD)],
            send_sem=out_send.at[turn, h],
            recv_sem=out_recv.at[turn, h],
            device_id=(cp, 2 * high + low),
            device_id_type=MESH,
        )

    def received(turn, h):
        high, low = peer_of(turn)
        return pltpu.make_async_remote_copy(
            src_ref=outs.at[turn, h],
            dst_ref=out_hbm.at[:, pl.ds(((2 * high + low) * heads + h) * HEAD, HEAD)],
            send_sem=out_send.at[turn, h],
            recv_sem=out_recv.at[turn, h],
            device_id=(cp, 2 * high + low),
            device_id_type=MESH,
        )

    def keep(h):
        return pltpu.make_async_copy(
            outs.at[3, h], out_hbm.at[:, pl.ds((tp * heads + h) * HEAD, HEAD)], own_sem.at[h]
        )

    for g in range(kv_local):
        for direction in range(2):
            for part in range(2):
                load(direction, g, part).start()
    for h in range(heads):
        load_q(h).start()

    barrier = pltpu.get_barrier_semaphore()
    for device in (beyond[0], beyond[1], partner):
        pl.semaphore_signal(barrier, inc=1, device_id=(device, tp), device_id_type=MESH)
    for turn in range(3):
        high, low = peer_of(turn)
        pl.semaphore_signal(barrier, inc=1, device_id=(cp, 2 * high + low), device_id_type=MESH)
    pl.semaphore_wait(barrier, 6)

    for g in range(kv_local):
        for direction in range(2):
            load(direction, g, 0).wait()
            load(direction, g, 1).wait()
            hop(direction, g, 0).start()

            @pl.when(is_lead[direction])
            def _():
                across(direction, g, 0).start()

    row = lax.broadcasted_iota(jnp.int32, (HEAD, HEAD), 0)
    col = lax.broadcasted_iota(jnp.int32, (HEAD, HEAD), 1)
    upper = (row <= col).astype(jnp.float32)
    lens = jnp.broadcast_to(lens_ref[...], (8, HEAD))
    ends = jnp.dot(lens, upper, precision=lax.Precision.HIGHEST, preferred_element_type=jnp.float32)[:1]
    lens = lens[:1]
    for turn in range(4):
        high, low = peer_of(turn)
        block = high * (2 * cp_size - 1 - 2 * cp) + cp
        q_pos = (
            lax.broadcasted_iota(jnp.int32, (chunk, 1), 0) + (block * half + low * chunk)
        ).astype(jnp.float32)
        start = jnp.sum(jnp.where(ends <= q_pos, lens, 0.0), axis=1, keepdims=True)
        for n in range(key_tiles):
            k_pos = (
                lax.broadcasted_iota(jnp.int32, (1, KEY_TILE), 1)
                + ((block - 4) * half + low * HEAD + n * KEY_TILE)
            ).astype(jnp.float32)
            allowed = (k_pos >= start) & (k_pos <= q_pos)
            bias[turn, :, n * KEY_TILE : (n + 1) * KEY_TILE] = jnp.where(allowed, 0.0, MASKED)

    for h in range(heads):
        load_q(h).wait()

    for g in range(kv_local):
        for direction in range(2):
            arrived(direction, g, 2)
            hop(direction, g, 1).start()

            @pl.when(is_lead[direction])
            def _():
                across(direction, g, 1).start()

            @pl.when(is_lead[1 - direction])
            def _():
                across(direction, g, 0).start()

    def complete(g):
        for direction in range(2):
            arrived(direction, g, 0)

            @pl.when(is_lead[1 - direction])
            def _():
                across(direction, g, 1).start()

        for direction in range(2):
            arrived(direction, g, 3)
            arrived(direction, g, 1)

    complete(0)

    factor = math.log2(math.e) / math.sqrt(HEAD)

    def unit(u, carry):
        later = u // 4
        turn = (1 - later) * (u % 2) + later * (2 + (u % 4) // 2)
        g = (1 - later) * (u // 2) + later * (u % 2)
        direction, low = peer_of(turn)
        q_start = pl.multiple_of(direction * half + low * chunk, 64)
        k_start = pl.multiple_of(low * HEAD, HEAD)

        @pl.when(u == 2)
        def _():
            for later_g in range(1, kv_local):
                complete(later_g)

        def scores_tile(h, n):
            q = qbuf[g * groups + h, pl.ds(q_start, chunk), :]
            k = kv[direction, g, 0, pl.ds(k_start + n * KEY_TILE, KEY_TILE), :]
            s = lax.dot_general(q, k, (((1,), (1,)), ((), ())), preferred_element_type=jnp.float32)
            s = s * factor + bias[turn, :, n * KEY_TILE : (n + 1) * KEY_TILE]
            scores[h % 2, :, n * KEY_TILE : (n + 1) * KEY_TILE] = s
            return jnp.maximum(s[:, :HEAD], s[:, HEAD:])

        def value_tile(h, n, top):
            p = jnp.exp2(scores[h % 2, :, n * KEY_TILE : (n + 1) * KEY_TILE] - top)
            v = kv[direction, g, 1, pl.ds(k_start + n * KEY_TILE, KEY_TILE), :]
            product = jnp.dot(p.astype(jnp.bfloat16), v, preferred_element_type=jnp.float32)
            return product, p[:, :HEAD] + p[:, HEAD:]

        highest = scores_tile(0, 0)
        for n in range(1, key_tiles):
            highest = jnp.maximum(highest, scores_tile(0, n))
        for h in range(groups):
            top = jnp.max(highest, axis=1, keepdims=True)
            total = weight = highest = None
            for n in range(key_tiles):
                if h + 1 < groups:
                    tile = scores_tile(h + 1, n)
                    highest = tile if highest is None else jnp.maximum(highest, tile)
                product, part = value_tile(h, n, top)
                total = product if total is None else total + product
                weight = part if weight is None else weight + part
            weight = jnp.sum(weight, axis=1, keepdims=True)
            outs[turn, g * groups + h] = (total / weight).astype(outs.dtype)
            if h > 0:
                ship(turn, g * groups + h - 1)
        ship(turn, g * groups + groups - 1)
        return carry

    def ship(turn, h):
        @pl.when(turn < 3)
        def _():
            send(turn, h).start()

        @pl.when(turn == 3)
        def _():
            keep(h).start()

    lax.fori_loop(0, 4 * kv_local, unit, 0)

    for g in range(kv_local):
        for direction in range(2):
            for far in range(2):
                hop(direction, g, far).wait_send()
                across(direction, g, far).wait_send()

    def drain(i, carry):
        turn, h = i // heads, i % heads
        send(turn, h).wait_send()
        received(turn, h).wait_recv()
        return carry

    lax.fori_loop(0, 3 * heads, drain, 0)
    for h in range(heads):
        keep(h).wait()


def on_device(cp_size, tp_size, queries, keys, values, doc_lengths):
    tok_rows, q_cols = queries.shape
    half = tok_rows // 2
    kv_local = keys.shape[1] // HEAD
    heads = q_cols // HEAD
    groups = heads // kv_local
    chunk = tok_rows // tp_size
    window = 7 * KEY_TILE
    lens = jnp.pad(doc_lengths.astype(jnp.float32), (0, HEAD - doc_lengths.shape[0]))[None]
    hbm = pl.BlockSpec(memory_space=pl.ANY)
    return pl.pallas_call(
        functools.partial(kernel, (cp_size, tp_size, half, groups, kv_local)),
        out_shape=jax.ShapeDtypeStruct((chunk, q_cols * tp_size), jnp.bfloat16),
        in_specs=[pl.BlockSpec(memory_space=pltpu.VMEM), hbm, hbm, hbm],
        out_specs=hbm,
        scratch_shapes=[
            pltpu.VMEM((2, kv_local, 2, 5 * half, HEAD), jnp.bfloat16),
            pltpu.VMEM((heads, tok_rows, HEAD), jnp.bfloat16),
            pltpu.VMEM((4, chunk, window), jnp.float32),
            pltpu.VMEM((2, chunk, window), jnp.float32),
            pltpu.VMEM((4, heads, chunk, HEAD), jnp.bfloat16),
            pltpu.SemaphoreType.DMA((2, kv_local, 2)),
            pltpu.SemaphoreType.DMA((heads,)),
            pltpu.SemaphoreType.DMA((2, kv_local, 4)),
            pltpu.SemaphoreType.DMA((2, kv_local, 4)),
            pltpu.SemaphoreType.DMA((3, heads)),
            pltpu.SemaphoreType.DMA((3, heads)),
            pltpu.SemaphoreType.DMA((heads,)),
        ],
        compiler_params=pltpu.CompilerParams(
            collective_id=0, has_side_effects=True, vmem_limit_bytes=60 * 1024 * 1024
        ),
    )(lens, queries, keys, values)


def solution(mesh):
    in_specs = (P("cp", "tp"), P("cp", "tp"), P("cp", "tp"), P())
    out_specs = P(("cp", "tp"), None)
    return jax.shard_map(
        functools.partial(on_device, mesh.shape["cp"], mesh.shape["tp"]),
        mesh=mesh, in_specs=in_specs, out_specs=out_specs, check_vma=False,
    )
```

```python
import functools
import math

import jax
import jax.numpy as jnp
from jax import lax
from jax.experimental import pallas as pl
from jax.experimental.pallas import tpu as pltpu
from jax.sharding import PartitionSpec as P

HEAD = 128
MESH = pl.DeviceIdType.MESH
MASKED = -1e30
KEY_TILE = 256


def kernel(sizes, lens_ref, q_hbm, k_hbm, v_hbm, out_hbm, kv, qbuf, bias, scores, outs,
           load_sem, q_sem, kv_send, leap_send, kv_recv, out_send, out_recv, own_sem):
    cp_size, tp_size, half, groups, kv_local = sizes
    heads = groups * kv_local
    chunk = 2 * half // tp_size
    window = bias.shape[-1]
    key_tiles = window // KEY_TILE
    cp = lax.axis_index("cp")
    tp = lax.axis_index("tp")
    core = cp % 2
    partner = cp + 1 - 2 * core

    def slot(direction, g, part, which):
        return kv.at[direction, g, part, pl.ds(which * half, half), :]

    at_end = [(cp >= cp_size - 2).astype(jnp.int32), (cp < 2).astype(jnp.int32)]
    beyond = [
        (1 - at_end[0]) * (cp + 2) + at_end[0] * partner,
        (1 - at_end[1]) * (cp - 2) + at_end[1] * partner,
    ]
    landing = [at_end[0], 1 - at_end[1]]
    is_lead = [core == 0, core == 1]
    lead_of = [1 - core, core]

    chips = cp_size // 2
    chip = cp // 2
    middle = chips // 2
    stops = [chip == middle - 1, chip == middle]
    leaps = [chip == middle - 2, chip == middle + 1]
    leap_to = [cp + 4, cp - 4]
    near_gap = (chip >= middle - 2) & (chip <= middle + 1)
    below_gap = (chip < middle).astype(jnp.int32)
    mate = cp - 4 + 8 * below_gap

    def load(direction, g, part):
        src = (k_hbm, v_hbm)[part]
        return pltpu.make_async_copy(
            src.at[pl.ds(direction * half, half), pl.ds(g * HEAD, HEAD)],
            slot(direction, g, part, 4),
            load_sem.at[direction, g, part],
        )

    def load_q(h):
        return pltpu.make_async_copy(
            q_hbm.at[:, pl.ds(h * HEAD, HEAD)], qbuf.at[h], q_sem.at[h]
        )

    def hop(direction, g, part, far):
        return pltpu.make_async_remote_copy(
            src_ref=slot(direction, g, part, 4 - 2 * far),
            dst_ref=slot(landing[direction], g, part, 2 - 2 * far),
            send_sem=kv_send.at[direction, g, part, far],
            recv_sem=kv_recv.at[landing[direction], g, part, 2 - 2 * far],
            device_id=(beyond[direction], tp),
            device_id_type=MESH,
        )

    def leap(direction, g, part):
        return pltpu.make_async_remote_copy(
            src_ref=slot(direction, g, part, 4),
            dst_ref=slot(direction, g, part, 0),
            send_sem=leap_send.at[direction, g, part],
            recv_sem=kv_recv.at[direction, g, part, 0],
            device_id=(leap_to[direction], tp),
            device_id_type=MESH,
        )

    def across(direction, g, part, far):
        lead = lead_of[direction]
        return pltpu.make_async_remote_copy(
            src_ref=slot(direction, g, part, 2 * lead + 2 - 2 * far),
            dst_ref=slot(direction, g, part, 3 - 2 * far),
            send_sem=kv_send.at[direction, g, part, 2 + far],
            recv_sem=kv_recv.at[direction, g, part, 3 - 2 * far],
            device_id=(partner, tp),
            device_id_type=MESH,
        )

    def arrived(direction, g, part, which):
        pltpu.make_async_remote_copy(
            src_ref=slot(direction, g, part, which),
            dst_ref=slot(direction, g, part, which),
            send_sem=kv_send.at[direction, g, part, 0],
            recv_sem=kv_recv.at[direction, g, part, which],
            device_id=(partner, tp),
            device_id_type=MESH,
        ).wait_recv()

    def offer(g, part):
        for direction in range(2):
            load(direction, g, part).wait()
            hop(direction, g, part, 0).start()

            @pl.when(leaps[direction])
            def _():
                leap(direction, g, part).start()

            @pl.when(is_lead[direction])
            def _():
                across(direction, g, part, 0).start()

    def relay(g, part):
        for direction in range(2):
            arrived(direction, g, part, 2)

            @pl.when(jnp.logical_not(stops[direction]))
            def _():
                hop(direction, g, part, 1).start()

            @pl.when(is_lead[direction])
            def _():
                across(direction, g, part, 1).start()

            @pl.when(is_lead[1 - direction])
            def _():
                across(direction, g, part, 0).start()

    def complete(g, part):
        for direction in range(2):
            arrived(direction, g, part, 0)

            @pl.when(is_lead[1 - direction])
            def _():
                across(direction, g, part, 1).start()

        for direction in range(2):
            arrived(direction, g, part, 3)
            arrived(direction, g, part, 1)

    def peer_of(turn):
        n = 3 - turn
        high = (tp // 2 + n // 2) % 2
        low = (tp % 2 + n % 2 + n // 2) % 2
        return high, low

    def send(turn, h):
        high, low = peer_of(turn)
        return pltpu.make_async_remote_copy(
            src_ref=outs.at[turn, h],
            dst_ref=out_hbm.at[:, pl.ds((tp * heads + h) * HEAD, HEAD)],
            send_sem=out_send.at[turn, h],
            recv_sem=out_recv.at[turn, h],
            device_id=(cp, 2 * high + low),
            device_id_type=MESH,
        )

    def received(turn, h):
        high, low = peer_of(turn)
        return pltpu.make_async_remote_copy(
            src_ref=outs.at[turn, h],
            dst_ref=out_hbm.at[:, pl.ds(((2 * high + low) * heads + h) * HEAD, HEAD)],
            send_sem=out_send.at[turn, h],
            recv_sem=out_recv.at[turn, h],
            device_id=(cp, 2 * high + low),
            device_id_type=MESH,
        )

    def keep(h):
        return pltpu.make_async_copy(
            outs.at[3, h], out_hbm.at[:, pl.ds((tp * heads + h) * HEAD, HEAD)], own_sem.at[h]
        )

    barrier = pltpu.get_barrier_semaphore()
    for turn in range(3):
        high, low = peer_of(turn)
        pl.semaphore_signal(barrier, inc=1, device_id=(cp, 2 * high + low), device_id_type=MESH)
    for device in (beyond[0], beyond[1], partner):
        pl.semaphore_signal(barrier, inc=1, device_id=(device, tp), device_id_type=MESH)

    @pl.when(near_gap)
    def _():
        pl.semaphore_signal(barrier, inc=1, device_id=(mate, tp), device_id_type=MESH)

    for g in range(kv_local):
        for part in range(2):
            for direction in range(2):
                load(direction, g, part).start()
    for h in range(heads):
        load_q(h).start()

    pl.semaphore_wait(barrier, 6 + near_gap.astype(jnp.int32))

    offer(0, 0)
    offer(0, 1)

    row = lax.broadcasted_iota(jnp.int32, (HEAD, HEAD), 0)
    col = lax.broadcasted_iota(jnp.int32, (HEAD, HEAD), 1)
    upper = (row <= col).astype(jnp.float32)
    lens = jnp.broadcast_to(lens_ref[...], (8, HEAD))
    ends = jnp.dot(lens, upper, precision=lax.Precision.HIGHEST, preferred_element_type=jnp.float32)[:1]
    lens = lens[:1]
    for turn in range(4):
        high, low = peer_of(turn)
        block = high * (2 * cp_size - 1 - 2 * cp) + cp
        q_pos = (
            lax.broadcasted_iota(jnp.int32, (chunk, 1), 0) + (block * half + low * chunk)
        ).astype(jnp.float32)
        start = jnp.sum(jnp.where(ends <= q_pos, lens, 0.0), axis=1, keepdims=True)
        for n in range(key_tiles):
            k_pos = (
                lax.broadcasted_iota(jnp.int32, (1, KEY_TILE), 1)
                + ((block - 4) * half + low * HEAD + n * KEY_TILE)
            ).astype(jnp.float32)
            allowed = (k_pos >= start) & (k_pos <= q_pos)
            bias[turn, :, n * KEY_TILE : (n + 1) * KEY_TILE] = jnp.where(allowed, 0.0, MASKED)

    for h in range(heads):
        load_q(h).wait()

    relay(0, 0)
    relay(0, 1)
    for g in range(1, kv_local):
        offer(g, 0)
        offer(g, 1)
    complete(0, 0)
    complete(0, 1)

    factor = math.log2(math.e) / math.sqrt(HEAD)

    def ship(turn, h):
        @pl.when(turn < 3)
        def _():
            send(turn, h).start()

        @pl.when(turn == 3)
        def _():
            keep(h).start()

    def place(u):
        later = u // 4
        turn = (1 - later) * (u % 2) + later * (2 + (u % 4) // 2)
        g = (1 - later) * (u // 2) + later * (u % 2)
        return turn, g

    def unit(u, carry):
        turn, g = place(u)
        direction, low = peer_of(turn)
        q_start = pl.multiple_of(direction * half + low * chunk, 64)
        k_start = pl.multiple_of(low * HEAD, HEAD)

        @pl.when(u == 1)
        def _():
            relay(1, 0)

        @pl.when(u == 2)
        def _():
            relay(1, 1)
            complete(1, 0)
            complete(1, 1)

        def scores_tile(h, n):
            q = qbuf[g * groups + h, pl.ds(q_start, chunk), :]
            k = kv[direction, g, 0, pl.ds(k_start + n * KEY_TILE, KEY_TILE), :]
            s = lax.dot_general(q, k, (((1,), (1,)), ((), ())), preferred_element_type=jnp.float32)
            s = s * factor + bias[turn, :, n * KEY_TILE : (n + 1) * KEY_TILE]
            scores[h % 2, :, n * KEY_TILE : (n + 1) * KEY_TILE] = s
            return jnp.maximum(s[:, :HEAD], s[:, HEAD:])

        def value_tile(h, n, top):
            p = jnp.exp2(scores[h % 2, :, n * KEY_TILE : (n + 1) * KEY_TILE] - top)
            v = kv[direction, g, 1, pl.ds(k_start + n * KEY_TILE, KEY_TILE), :]
            product = jnp.dot(p.astype(jnp.bfloat16), v, preferred_element_type=jnp.float32)
            return product, p[:, :HEAD] + p[:, HEAD:]

        highest = scores_tile(0, 0)
        for n in range(1, key_tiles):
            highest = jnp.maximum(highest, scores_tile(0, n))

        @pl.when(u > 0)
        def _():
            last_turn, last_g = place(u - 1)
            ship(last_turn, last_g * groups + groups - 1)

        for h in range(groups):
            top = jnp.max(highest, axis=1, keepdims=True)
            total = weight = highest = None
            for n in range(key_tiles):
                if h + 1 < groups:
                    tile = scores_tile(h + 1, n)
                    highest = tile if highest is None else jnp.maximum(highest, tile)
                product, part = value_tile(h, n, top)
                total = product if total is None else total + product
                weight = part if weight is None else weight + part
            weight = jnp.sum(weight, axis=1, keepdims=True)
            outs[turn, g * groups + h] = (total / weight).astype(outs.dtype)
            if h > 0:
                ship(turn, g * groups + h - 1)
        return carry

    lax.fori_loop(0, 4 * kv_local, unit, 0)

    keep(heads - 1).start()

    for g in range(kv_local):
        for part in range(2):
            for direction in range(2):
                hop(direction, g, part, 0).wait_send()
                across(direction, g, part, 0).wait_send()
                across(direction, g, part, 1).wait_send()

                @pl.when(jnp.logical_not(stops[direction]))
                def _():
                    hop(direction, g, part, 1).wait_send()

                @pl.when(leaps[direction])
                def _():
                    leap(direction, g, part).wait_send()

    def drain(i, carry):
        turn, h = i // heads, i % heads
        send(turn, h).wait_send()
        received(turn, h).wait_recv()
        return carry

    lax.fori_loop(0, 3 * heads, drain, 0)
    for h in range(heads):
        keep(h).wait()


def on_device(cp_size, tp_size, queries, keys, values, doc_lengths):
    tok_rows, q_cols = queries.shape
    half = tok_rows // 2
    kv_local = keys.shape[1] // HEAD
    heads = q_cols // HEAD
    groups = heads // kv_local
    chunk = tok_rows // tp_size
    window = 7 * KEY_TILE
    lens = jnp.pad(doc_lengths.astype(jnp.float32), (0, HEAD - doc_lengths.shape[0]))[None]
    hbm = pl.BlockSpec(memory_space=pl.ANY)
    return pl.pallas_call(
        functools.partial(kernel, (cp_size, tp_size, half, groups, kv_local)),
        out_shape=jax.ShapeDtypeStruct((chunk, q_cols * tp_size), jnp.bfloat16),
        in_specs=[pl.BlockSpec(memory_space=pltpu.VMEM), hbm, hbm, hbm],
        out_specs=hbm,
        scratch_shapes=[
            pltpu.VMEM((2, kv_local, 2, 5 * half, HEAD), jnp.bfloat16),
            pltpu.VMEM((heads, tok_rows, HEAD), jnp.bfloat16),
            pltpu.VMEM((4, chunk, window), jnp.float32),
            pltpu.VMEM((2, chunk, window), jnp.float32),
            pltpu.VMEM((4, heads, chunk, HEAD), jnp.bfloat16),
            pltpu.SemaphoreType.DMA((2, kv_local, 2)),
            pltpu.SemaphoreType.DMA((heads,)),
            pltpu.SemaphoreType.DMA((2, kv_local, 2, 4)),
            pltpu.SemaphoreType.DMA((2, kv_local, 2)),
            pltpu.SemaphoreType.DMA((2, kv_local, 2, 4)),
            pltpu.SemaphoreType.DMA((3, heads)),
            pltpu.SemaphoreType.DMA((3, heads)),
            pltpu.SemaphoreType.DMA((heads,)),
        ],
        compiler_params=pltpu.CompilerParams(
            collective_id=0, has_side_effects=True, vmem_limit_bytes=60 * 1024 * 1024
        ),
    )(lens, queries, keys, values)


def solution(mesh):
    in_specs = (P("cp", "tp"), P("cp", "tp"), P("cp", "tp"), P())
    out_specs = P(("cp", "tp"), None)
    return jax.shard_map(
        functools.partial(on_device, mesh.shape["cp"], mesh.shape["tp"]),
        mesh=mesh, in_specs=in_specs, out_specs=out_specs, check_vma=False,
    )
```

```python
import functools
import math

import jax
import jax.numpy as jnp
from jax import lax
from jax.experimental import pallas as pl
from jax.experimental.pallas import tpu as pltpu
from jax.sharding import PartitionSpec as P

HEAD = 128
MESH = pl.DeviceIdType.MESH
MASKED = -1e30
KEY_TILE = 256


def kernel(sizes, lens_ref, q_hbm, k_hbm, v_hbm, out_hbm, kv, qbuf, bias, scores, outs,
           load_sem, q_sem, kv_send, leap_send, kv_recv, out_send, out_recv, own_sem):
    cp_size, tp_size, half, groups, kv_local = sizes
    heads = groups * kv_local
    chunk = 2 * half // tp_size
    window = bias.shape[-1]
    key_tiles = window // KEY_TILE
    cp = lax.axis_index("cp")
    tp = lax.axis_index("tp")
    core = cp % 2
    partner = cp + 1 - 2 * core
    far_way = 1 - tp // 2
    near_way = tp // 2

    def slot(direction, g, part, which):
        return kv.at[direction, g, part, pl.ds(which * half, half), :]

    at_top = (cp >= cp_size - 2).astype(jnp.int32)
    at_bottom = (cp < 2).astype(jnp.int32)
    is_end = ((cp < 2) & (far_way == 0)) | ((cp >= cp_size - 2) & (far_way == 1))
    above = (1 - at_top) * (cp + 2) + at_top * partner
    below = (1 - at_bottom) * (cp - 2) + at_bottom * partner

    chips = cp_size // 2
    chip = cp // 2
    middle = chips // 2
    near_gap = (chip >= middle - 2) & (chip <= middle + 1)
    below_gap = (chip < middle).astype(jnp.int32)
    mate = cp - 4 + 8 * below_gap
    near_first = near_gap & (near_way == 1 - below_gap)

    def beyond(direction):
        return (1 - direction) * above + direction * below

    def landing(direction):
        return (1 - direction) * at_top + direction * (1 - at_bottom)

    def lead(direction):
        return (1 - core) * (1 - direction) + core * direction

    def stops(direction):
        return chip == middle - 1 + direction

    def leaps(direction):
        return chip == middle - 2 + 3 * direction

    def load(direction, g, part):
        src = (k_hbm, v_hbm)[part]
        return pltpu.make_async_copy(
            src.at[pl.ds(pl.multiple_of(direction * half, half), half), pl.ds(g * HEAD, HEAD)],
            slot(direction, g, part, 4),
            load_sem.at[direction, g, part],
        )

    def load_q(h):
        return pltpu.make_async_copy(
            q_hbm.at[:, pl.ds(h * HEAD, HEAD)], qbuf.at[h], q_sem.at[h]
        )

    def hop(direction, g, part, far):
        return pltpu.make_async_remote_copy(
            src_ref=slot(direction, g, part, 4 - 2 * far),
            dst_ref=slot(landing(direction), g, part, 2 - 2 * far),
            send_sem=kv_send.at[direction, g, part, far],
            recv_sem=kv_recv.at[landing(direction), g, part, 2 - 2 * far],
            device_id=(beyond(direction), tp),
            device_id_type=MESH,
        )

    def leap(direction, g, part):
        return pltpu.make_async_remote_copy(
            src_ref=slot(direction, g, part, 4),
            dst_ref=slot(direction, g, part, 0),
            send_sem=leap_send.at[direction, g, part],
            recv_sem=kv_recv.at[direction, g, part, 0],
            device_id=(cp + 4 - 8 * direction, tp),
            device_id_type=MESH,
        )

    def across(direction, g, part, far):
        return pltpu.make_async_remote_copy(
            src_ref=slot(direction, g, part, 2 * lead(direction) + 2 - 2 * far),
            dst_ref=slot(direction, g, part, 3 - 2 * far),
            send_sem=kv_send.at[direction, g, part, 2 + far],
            recv_sem=kv_recv.at[direction, g, part, 3 - 2 * far],
            device_id=(partner, tp),
            device_id_type=MESH,
        )

    def arrived(direction, g, part, which):
        pltpu.make_async_remote_copy(
            src_ref=slot(direction, g, part, which),
            dst_ref=slot(direction, g, part, which),
            send_sem=kv_send.at[direction, g, part, 0],
            recv_sem=kv_recv.at[direction, g, part, which],
            device_id=(partner, tp),
            device_id_type=MESH,
        ).wait_recv()

    def offer(direction, g, part):
        load(direction, g, part).wait()
        hop(direction, g, part, 0).start()

        @pl.when(leaps(direction))
        def _():
            leap(direction, g, part).start()

        @pl.when(lead(direction) == 1)
        def _():
            across(direction, g, part, 0).start()

    def relay(direction, g, part):
        arrived(direction, g, part, 2)

        @pl.when(jnp.logical_not(stops(direction)))
        def _():
            hop(direction, g, part, 1).start()

        @pl.when(lead(direction) == 1)
        def _():
            across(direction, g, part, 1).start()

        @pl.when(lead(direction) == 0)
        def _():
            across(direction, g, part, 0).start()

    def complete(direction, g, part):
        arrived(direction, g, part, 0)

        @pl.when(lead(direction) == 0)
        def _():
            across(direction, g, part, 1).start()

        arrived(direction, g, part, 3)
        arrived(direction, g, part, 1)

    def peer_of(turn):
        n = 3 - turn
        high = (tp // 2 + n // 2) % 2
        low = (tp % 2 + n % 2 + n // 2) % 2
        return high, low

    def send(turn, h):
        high, low = peer_of(turn)
        return pltpu.make_async_remote_copy(
            src_ref=outs.at[turn, h],
            dst_ref=out_hbm.at[:, pl.ds((tp * heads + h) * HEAD, HEAD)],
            send_sem=out_send.at[turn, h],
            recv_sem=out_recv.at[turn, h],
            device_id=(cp, 2 * high + low),
            device_id_type=MESH,
        )

    def received(turn, h):
        high, low = peer_of(turn)
        return pltpu.make_async_remote_copy(
            src_ref=outs.at[turn, h],
            dst_ref=out_hbm.at[:, pl.ds(((2 * high + low) * heads + h) * HEAD, HEAD)],
            send_sem=out_send.at[turn, h],
            recv_sem=out_recv.at[turn, h],
            device_id=(cp, 2 * high + low),
            device_id_type=MESH,
        )

    def keep(h):
        return pltpu.make_async_copy(
            outs.at[3, h], out_hbm.at[:, pl.ds((tp * heads + h) * HEAD, HEAD)], own_sem.at[h]
        )

    barrier = pltpu.get_barrier_semaphore()
    for turn in range(3):
        high, low = peer_of(turn)
        pl.semaphore_signal(barrier, inc=1, device_id=(cp, 2 * high + low), device_id_type=MESH)
    for device in (above, below, partner):
        pl.semaphore_signal(barrier, inc=1, device_id=(device, tp), device_id_type=MESH)

    @pl.when(near_gap)
    def _():
        pl.semaphore_signal(barrier, inc=1, device_id=(mate, tp), device_id_type=MESH)

    for direction in (far_way, near_way):
        for g in range(kv_local):
            for part in range(2):
                load(direction, g, part).start()
    for h in range(heads):
        load_q(h).start()

    pl.semaphore_wait(barrier, 6 + near_gap.astype(jnp.int32))

    offer(far_way, 0, 0)
    offer(far_way, 0, 1)

    @pl.when(jnp.logical_not(near_gap))
    def _():
        offer(near_way, 0, 0)
        offer(near_way, 0, 1)


    row = lax.broadcasted_iota(jnp.int32, (HEAD, HEAD), 0)
    col = lax.broadcasted_iota(jnp.int32, (HEAD, HEAD), 1)
    upper = (row <= col).astype(jnp.float32)
    docs = lens_ref.shape[-1]
    lens = jnp.concatenate(
        [lens_ref[...].reshape(1, docs).astype(jnp.float32), jnp.zeros((1, HEAD - docs), jnp.float32)], axis=1
    )
    lens = jnp.broadcast_to(lens, (8, HEAD))
    ends = jnp.dot(lens, upper, precision=lax.Precision.HIGHEST, preferred_element_type=jnp.float32)[:1]
    lens = lens[:1]
    for turn in range(4):
        high, low = peer_of(turn)
        block = high * (2 * cp_size - 1 - 2 * cp) + cp
        q_pos = (
            lax.broadcasted_iota(jnp.int32, (chunk, 1), 0) + (block * half + low * chunk)
        ).astype(jnp.float32)
        start = jnp.sum(jnp.where(ends <= q_pos, lens, 0.0), axis=1, keepdims=True)
        for n in range(key_tiles):
            k_pos = (
                lax.broadcasted_iota(jnp.int32, (1, KEY_TILE), 1)
                + ((block - 4) * half + low * HEAD + n * KEY_TILE)
            ).astype(jnp.float32)
            allowed = (k_pos >= start) & (k_pos <= q_pos)
            bias[turn, :, n * KEY_TILE : (n + 1) * KEY_TILE] = jnp.where(allowed, 0.0, MASKED)

    for h in range(heads):
        load_q(h).wait()

    @pl.when(near_gap)
    def _():
        hop(far_way, 0, 1, 0).wait_send()
        for way, g in ((near_way, 0), (far_way, 1), (near_way, 1)):
            offer(way, g, 0)
            offer(way, g, 1)

    @pl.when(near_first)
    def _():
        for g in range(kv_local):
            relay(near_way, g, 0)
            relay(near_way, g, 1)

    relay(far_way, 0, 0)
    relay(far_way, 0, 1)

    @pl.when(jnp.logical_not(near_gap))
    def _():
        for way in (far_way, near_way):
            offer(way, 1, 0)
            offer(way, 1, 1)

    @pl.when(is_end)
    def _():
        relay(near_way, 0, 0)
        relay(near_way, 0, 1)

    complete(far_way, 0, 0)

    factor = math.log2(math.e) / math.sqrt(HEAD)

    def ship(turn, h):
        @pl.when(turn < 3)
        def _():
            send(turn, h).start()

        @pl.when(turn == 3)
        def _():
            keep(h).start()

    def place(u):
        return 2 * (u // 4) + u % 2, (u // 2) % 2

    def unit(u, carry):
        turn, g = place(u)
        direction, low = peer_of(turn)
        q_start = pl.multiple_of(direction * half + low * chunk, 64)
        k_start = pl.multiple_of(low * HEAD, HEAD)

        @pl.when(u == 1)
        def _():
            relay(far_way, 1, 0)
            relay(far_way, 1, 1)

        @pl.when(u == 2)
        def _():
            @pl.when(is_end)
            def _():
                relay(near_way, 1, 0)
                relay(near_way, 1, 1)

            complete(far_way, 1, 0)
            complete(far_way, 1, 1)

            @pl.when(jnp.logical_not(is_end | near_first))
            def _():
                relay(near_way, 0, 0)
                relay(near_way, 0, 1)

        @pl.when((u == 3) & jnp.logical_not(is_end | near_first))
        def _():
            relay(near_way, 1, 0)
            relay(near_way, 1, 1)

        @pl.when(u == 4)
        def _():
            complete(near_way, 0, 0)
            complete(near_way, 0, 1)

        @pl.when(u == 6)
        def _():
            complete(near_way, 1, 0)
            complete(near_way, 1, 1)

        def scores_tile(h, n):
            q = qbuf[g * groups + h, pl.ds(q_start, chunk), :]
            k = kv[direction, g, 0, pl.ds(k_start + n * KEY_TILE, KEY_TILE), :]
            s = lax.dot_general(q, k, (((1,), (1,)), ((), ())), preferred_element_type=jnp.float32)
            s = s * factor + bias[turn, :, n * KEY_TILE : (n + 1) * KEY_TILE]
            scores[h % 2, :, n * KEY_TILE : (n + 1) * KEY_TILE] = s
            return jnp.maximum(s[:, :HEAD], s[:, HEAD:])

        def value_tile(h, n, top):
            p = jnp.exp2(scores[h % 2, :, n * KEY_TILE : (n + 1) * KEY_TILE] - top)
            v = kv[direction, g, 1, pl.ds(k_start + n * KEY_TILE, KEY_TILE), :]
            product = jnp.dot(p.astype(jnp.bfloat16), v, preferred_element_type=jnp.float32)
            return product, p[:, :HEAD] + p[:, HEAD:]

        highest = scores_tile(0, 0)
        for n in range(1, key_tiles):
            highest = jnp.maximum(highest, scores_tile(0, n))

        @pl.when(u == 0)
        def _():
            complete(far_way, 0, 1)

        @pl.when(u > 0)
        def _():
            last_turn, last_g = place(u - 1)
            ship(last_turn, last_g * groups + groups - 1)

        for h in range(groups):
            top = jnp.max(highest, axis=1, keepdims=True)
            total = weight = highest = None
            for n in range(key_tiles):
                if h + 1 < groups:
                    tile = scores_tile(h + 1, n)
                    highest = tile if highest is None else jnp.maximum(highest, tile)
                product, part = value_tile(h, n, top)
                total = product if total is None else total + product
                weight = part if weight is None else weight + part
            weight = jnp.sum(weight, axis=1, keepdims=True)
            outs[turn, g * groups + h] = (total / weight).astype(outs.dtype)
            if h > 0:
                ship(turn, g * groups + h - 1)
        return carry

    lax.fori_loop(0, 4 * kv_local, unit, 0)

    keep(heads - 1).start()

    for g in range(kv_local):
        for part in range(2):
            for way in (far_way, near_way):
                if g == 0 and part == 1 and way is far_way:

                    @pl.when(jnp.logical_not(near_gap))
                    def _():
                        hop(way, g, part, 0).wait_send()

                else:
                    hop(way, g, part, 0).wait_send()
                across(way, g, part, 0).wait_send()
                across(way, g, part, 1).wait_send()

                @pl.when(jnp.logical_not(stops(way)))
                def _():
                    hop(way, g, part, 1).wait_send()

                @pl.when(leaps(way))
                def _():
                    leap(way, g, part).wait_send()

    def drain(i, carry):
        turn, h = i // heads, i % heads
        send(turn, h).wait_send()
        received(turn, h).wait_recv()
        return carry

    lax.fori_loop(0, 3 * heads, drain, 0)
    for h in range(heads):
        keep(h).wait()


def on_device(cp_size, tp_size, queries, keys, values, doc_lengths):
    tok_rows, q_cols = queries.shape
    half = tok_rows // 2
    kv_local = keys.shape[1] // HEAD
    heads = q_cols // HEAD
    groups = heads // kv_local
    chunk = tok_rows // tp_size
    window = 7 * KEY_TILE
    hbm = pl.BlockSpec(memory_space=pl.ANY)
    return pl.pallas_call(
        functools.partial(kernel, (cp_size, tp_size, half, groups, kv_local)),
        out_shape=pltpu.VMEM((chunk, q_cols * tp_size), jnp.bfloat16),
        in_specs=[pl.BlockSpec(memory_space=pltpu.VMEM), hbm, hbm, hbm],
        out_specs=pl.BlockSpec(memory_space=pltpu.VMEM),
        scratch_shapes=[
            pltpu.VMEM((2, kv_local, 2, 5 * half, HEAD), jnp.bfloat16),
            pltpu.VMEM((heads, tok_rows, HEAD), jnp.bfloat16),
            pltpu.VMEM((4, chunk, window), jnp.float32),
            pltpu.VMEM((2, chunk, window), jnp.float32),
            pltpu.VMEM((4, heads, chunk, HEAD), jnp.bfloat16),
            pltpu.SemaphoreType.DMA((2, kv_local, 2)),
            pltpu.SemaphoreType.DMA((heads,)),
            pltpu.SemaphoreType.DMA((2, kv_local, 2, 4)),
            pltpu.SemaphoreType.DMA((2, kv_local, 2)),
            pltpu.SemaphoreType.DMA((2, kv_local, 2, 4)),
            pltpu.SemaphoreType.DMA((3, heads)),
            pltpu.SemaphoreType.DMA((3, heads)),
            pltpu.SemaphoreType.DMA((heads,)),
        ],
        compiler_params=pltpu.CompilerParams(
            collective_id=0, has_side_effects=True, vmem_limit_bytes=60 * 1024 * 1024
        ),
    )(doc_lengths, queries, keys, values)


def solution(mesh):
    in_specs = (P("cp", "tp"), P("cp", "tp"), P("cp", "tp"), P())
    out_specs = P(("cp", "tp"), None)
    return jax.shard_map(
        functools.partial(on_device, mesh.shape["cp"], mesh.shape["tp"]),
        mesh=mesh, in_specs=in_specs, out_specs=out_specs, check_vma=False,
    )
```

```python
import functools
import math

import jax
import jax.numpy as jnp
from jax import lax
from jax.experimental import pallas as pl
from jax.experimental.pallas import tpu as pltpu
from jax.sharding import PartitionSpec as P

HEAD = 128
MESH = pl.DeviceIdType.MESH
MASKED = -1e30
KEY_TILE = 256


def kernel(sizes, lens_ref, q_hbm, k_hbm, v_hbm, out_hbm, kv, passing, qbuf, bias, scores, outs,
           load_sem, q_sem, kv_send, leap_send, kv_recv, pass_send, pass_recv, out_send, out_recv, own_sem):
    cp_size, tp_size, half, groups, kv_local = sizes
    heads = groups * kv_local
    chunk = 2 * half // tp_size
    window = bias.shape[-1]
    key_tiles = window // KEY_TILE
    cp = lax.axis_index("cp")
    tp = lax.axis_index("tp")
    core = cp % 2
    partner = cp + 1 - 2 * core
    far_way = 1 - tp // 2
    near_way = tp // 2

    def slot(direction, g, part, which):
        return kv.at[direction, g, part, pl.ds(which * half, half), :]

    at_top = (cp >= cp_size - 2).astype(jnp.int32)
    at_bottom = (cp < 2).astype(jnp.int32)
    is_end = ((cp < 2) & (far_way == 0)) | ((cp >= cp_size - 2) & (far_way == 1))
    above = (1 - at_top) * (cp + 2) + at_top * partner
    below = (1 - at_bottom) * (cp - 2) + at_bottom * partner

    chips = cp_size // 2
    chip = cp // 2
    middle = chips // 2
    near_gap = (chip >= middle - 2) & (chip <= middle + 1)
    below_gap = (chip < middle).astype(jnp.int32)
    mate = cp - 4 + 8 * below_gap
    near_first = near_gap & (near_way == 1 - below_gap)

    wrap = middle - math.isqrt(middle)
    odd = core == 1
    upper_relay = chip - middle - wrap
    lower_relay = middle - 1 - wrap - chip
    relays_up = odd & (lower_relay >= 0) & (lower_relay <= 1)
    relays_down = odd & (upper_relay >= 0) & (upper_relay <= 1)
    is_relay = relays_up | relays_down
    down = relays_down.astype(jnp.int32)
    relay_slot = 2 - 2 * ((1 - down) * lower_relay + down * upper_relay)
    relay_target = 2 * (middle - down) + 1
    relay_source = cp + 2 * wrap * (1 - 2 * down)
    detour_chip = odd & near_gap
    is_target = odd & ((chip == middle - 1) | (chip == middle))
    detour_via = cp - 2 * wrap * (2 * below_gap - 1)

    def beyond(direction):
        return (1 - direction) * above + direction * below

    def landing(direction):
        return (1 - direction) * at_top + direction * (1 - at_bottom)

    def lead(direction):
        return (1 - core) * (1 - direction) + core * direction

    def stops(direction):
        return chip == middle - 1 + direction

    def leaps(direction):
        return (chip == middle - 2 + 3 * direction) & (core == 0)

    def detours(direction):
        return odd & (stops(direction) | (chip == middle - 2 + 3 * direction))

    def hops(direction):
        return jnp.logical_not(odd & stops(direction))

    def load(direction, g, part):
        src = (k_hbm, v_hbm)[part]
        return pltpu.make_async_copy(
            src.at[pl.ds(pl.multiple_of(direction * half, half), half), pl.ds(g * HEAD, HEAD)],
            slot(direction, g, part, 4),
            load_sem.at[direction, g, part],
        )

    def load_q(h):
        return pltpu.make_async_copy(
            q_hbm.at[:, pl.ds(h * HEAD, HEAD)], qbuf.at[h], q_sem.at[h]
        )

    def hop(direction, g, part, far):
        return pltpu.make_async_remote_copy(
            src_ref=slot(direction, g, part, 4 - 2 * far),
            dst_ref=slot(landing(direction), g, part, 2 - 2 * far),
            send_sem=kv_send.at[direction, g, part, far],
            recv_sem=kv_recv.at[landing(direction), g, part, 2 - 2 * far],
            device_id=(beyond(direction), tp),
            device_id_type=MESH,
        )

    def leap(direction, g, part):
        return pltpu.make_async_remote_copy(
            src_ref=slot(direction, g, part, 4),
            dst_ref=slot(direction, g, part, 0),
            send_sem=leap_send.at[direction, g, part],
            recv_sem=kv_recv.at[direction, g, part, 0],
            device_id=(cp + 4 - 8 * direction, tp),
            device_id_type=MESH,
        )

    def detour(g, part):
        return pltpu.make_async_remote_copy(
            src_ref=slot(1 - below_gap, g, part, 4),
            dst_ref=passing.at[g, part],
            send_sem=leap_send.at[1 - below_gap, g, part],
            recv_sem=pass_recv.at[g, part],
            device_id=(detour_via, tp),
            device_id_type=MESH,
        )

    def forward(g, part):
        return pltpu.make_async_remote_copy(
            src_ref=passing.at[g, part],
            dst_ref=slot(down, g, part, relay_slot),
            send_sem=pass_send.at[g, part],
            recv_sem=kv_recv.at[down, g, part, relay_slot],
            device_id=(relay_target, tp),
            device_id_type=MESH,
        )

    def across(direction, g, part, far):
        return pltpu.make_async_remote_copy(
            src_ref=slot(direction, g, part, 2 * lead(direction) + 2 - 2 * far),
            dst_ref=slot(direction, g, part, 3 - 2 * far),
            send_sem=kv_send.at[direction, g, part, 2 + far],
            recv_sem=kv_recv.at[direction, g, part, 3 - 2 * far],
            device_id=(partner, tp),
            device_id_type=MESH,
        )

    def arrived(direction, g, part, which):
        pltpu.make_async_remote_copy(
            src_ref=slot(direction, g, part, which),
            dst_ref=slot(direction, g, part, which),
            send_sem=kv_send.at[direction, g, part, 0],
            recv_sem=kv_recv.at[direction, g, part, which],
            device_id=(partner, tp),
            device_id_type=MESH,
        ).wait_recv()

    def offer(direction, g, part):
        load(direction, g, part).wait()

        @pl.when(hops(direction))
        def _():
            hop(direction, g, part, 0).start()

        @pl.when(detours(direction))
        def _():
            detour(g, part).start()

        @pl.when(leaps(direction))
        def _():
            leap(direction, g, part).start()

        @pl.when(lead(direction) == 1)
        def _():
            across(direction, g, part, 0).start()

    def relay(direction, g, part):
        arrived(direction, g, part, 2)

        @pl.when(jnp.logical_not(stops(direction)))
        def _():
            hop(direction, g, part, 1).start()

        @pl.when(lead(direction) == 1)
        def _():
            across(direction, g, part, 1).start()

        @pl.when(lead(direction) == 0)
        def _():
            across(direction, g, part, 0).start()

    def complete(direction, g, part):
        arrived(direction, g, part, 0)

        @pl.when(lead(direction) == 0)
        def _():
            across(direction, g, part, 1).start()

        arrived(direction, g, part, 3)
        arrived(direction, g, part, 1)

    def peer_of(turn):
        n = 3 - turn
        high = (tp // 2 + n // 2) % 2
        low = (tp % 2 + n % 2 + n // 2) % 2
        return high, low

    def send(turn, h):
        high, low = peer_of(turn)
        return pltpu.make_async_remote_copy(
            src_ref=outs.at[turn, h],
            dst_ref=out_hbm.at[:, pl.ds((tp * heads + h) * HEAD, HEAD)],
            send_sem=out_send.at[turn, h],
            recv_sem=out_recv.at[turn, h],
            device_id=(cp, 2 * high + low),
            device_id_type=MESH,
        )

    def received(turn, h):
        high, low = peer_of(turn)
        return pltpu.make_async_remote_copy(
            src_ref=outs.at[turn, h],
            dst_ref=out_hbm.at[:, pl.ds(((2 * high + low) * heads + h) * HEAD, HEAD)],
            send_sem=out_send.at[turn, h],
            recv_sem=out_recv.at[turn, h],
            device_id=(cp, 2 * high + low),
            device_id_type=MESH,
        )

    def keep(h):
        return pltpu.make_async_copy(
            outs.at[3, h], out_hbm.at[:, pl.ds((tp * heads + h) * HEAD, HEAD)], own_sem.at[h]
        )

    barrier = pltpu.get_barrier_semaphore()
    for turn in range(3):
        high, low = peer_of(turn)
        pl.semaphore_signal(barrier, inc=1, device_id=(cp, 2 * high + low), device_id_type=MESH)
    for device in (above, below, partner):
        pl.semaphore_signal(barrier, inc=1, device_id=(device, tp), device_id_type=MESH)

    @pl.when(near_gap)
    def _():
        pl.semaphore_signal(barrier, inc=1, device_id=(mate, tp), device_id_type=MESH)

    @pl.when(detour_chip)
    def _():
        pl.semaphore_signal(barrier, inc=1, device_id=(detour_via, tp), device_id_type=MESH)

    @pl.when(is_relay)
    def _():
        for device in (relay_source, relay_target):
            pl.semaphore_signal(barrier, inc=1, device_id=(device, tp), device_id_type=MESH)

    @pl.when(is_target)
    def _():
        for step in range(2):
            low_relay = middle - 1 - wrap - step
            high_relay = middle + wrap + step
            device = 2 * (below_gap * high_relay + (1 - below_gap) * low_relay) + 1
            pl.semaphore_signal(barrier, inc=1, device_id=(device, tp), device_id_type=MESH)

    for direction in (far_way, near_way):
        for g in range(kv_local):
            for part in range(2):
                load(direction, g, part).start()
    for h in range(heads):
        load_q(h).start()

    greetings = (
        6 + near_gap.astype(jnp.int32) + detour_chip.astype(jnp.int32)
        + 2 * is_relay.astype(jnp.int32) + 2 * is_target.astype(jnp.int32)
    )
    pl.semaphore_wait(barrier, greetings)

    offer(far_way, 0, 0)
    offer(far_way, 0, 1)

    offer(near_way, 0, 0)
    offer(near_way, 0, 1)

    @pl.when(near_gap)
    def _():
        for way in (far_way, near_way):
            offer(way, 1, 0)
            offer(way, 1, 1)

    row = lax.broadcasted_iota(jnp.int32, (HEAD, HEAD), 0)
    col = lax.broadcasted_iota(jnp.int32, (HEAD, HEAD), 1)
    upper = (row <= col).astype(jnp.float32)
    docs = lens_ref.shape[-1]
    lens = jnp.concatenate(
        [lens_ref[...].reshape(1, docs).astype(jnp.float32), jnp.zeros((1, HEAD - docs), jnp.float32)], axis=1
    )
    lens = jnp.broadcast_to(lens, (8, HEAD))
    ends = jnp.dot(lens, upper, precision=lax.Precision.HIGHEST, preferred_element_type=jnp.float32)[:1]
    lens = lens[:1]
    for turn in range(4):
        high, low = peer_of(turn)
        block = high * (2 * cp_size - 1 - 2 * cp) + cp
        q_pos = (
            lax.broadcasted_iota(jnp.int32, (chunk, 1), 0) + (block * half + low * chunk)
        ).astype(jnp.float32)
        start = jnp.sum(jnp.where(ends <= q_pos, lens, 0.0), axis=1, keepdims=True)
        for n in range(key_tiles):
            k_pos = (
                lax.broadcasted_iota(jnp.int32, (1, KEY_TILE), 1)
                + ((block - 4) * half + low * HEAD + n * KEY_TILE)
            ).astype(jnp.float32)
            allowed = (k_pos >= start) & (k_pos <= q_pos)
            bias[turn, :, n * KEY_TILE : (n + 1) * KEY_TILE] = jnp.where(allowed, 0.0, MASKED)

    for h in range(heads):
        load_q(h).wait()

    @pl.when(near_first)
    def _():
        for g in range(kv_local):
            relay(near_way, g, 0)
            relay(near_way, g, 1)

    relay(far_way, 0, 0)
    relay(far_way, 0, 1)

    @pl.when(jnp.logical_not(near_gap))
    def _():
        for way in (far_way, near_way):
            offer(way, 1, 0)
            offer(way, 1, 1)

    @pl.when(is_relay)
    def _():
        for g in range(kv_local):
            for part in range(2):
                pltpu.make_async_remote_copy(
                    src_ref=passing.at[g, part],
                    dst_ref=passing.at[g, part],
                    send_sem=pass_send.at[g, part],
                    recv_sem=pass_recv.at[g, part],
                    device_id=(relay_source, tp),
                    device_id_type=MESH,
                ).wait_recv()
                forward(g, part).start()

    @pl.when(is_end)
    def _():
        relay(near_way, 0, 0)
        relay(near_way, 0, 1)

    complete(far_way, 0, 0)

    factor = math.log2(math.e) / math.sqrt(HEAD)

    def ship(turn, h):
        @pl.when(turn < 3)
        def _():
            send(turn, h).start()

        @pl.when(turn == 3)
        def _():
            keep(h).start()

    def place(u):
        return 2 * (u // 4) + u % 2, (u // 2) % 2

    def unit(u, carry):
        turn, g = place(u)
        direction, low = peer_of(turn)
        q_start = pl.multiple_of(direction * half + low * chunk, 64)
        k_start = pl.multiple_of(low * HEAD, HEAD)

        @pl.when(u == 1)
        def _():
            relay(far_way, 1, 0)
            relay(far_way, 1, 1)

        @pl.when(u == 2)
        def _():
            @pl.when(is_end)
            def _():
                relay(near_way, 1, 0)
                relay(near_way, 1, 1)

            complete(far_way, 1, 0)
            complete(far_way, 1, 1)

            @pl.when(jnp.logical_not(is_end | near_first))
            def _():
                relay(near_way, 0, 0)
                relay(near_way, 0, 1)

        @pl.when((u == 3) & jnp.logical_not(is_end | near_first))
        def _():
            relay(near_way, 1, 0)
            relay(near_way, 1, 1)

        @pl.when(u == 4)
        def _():
            complete(near_way, 0, 0)
            complete(near_way, 0, 1)

        @pl.when(u == 6)
        def _():
            complete(near_way, 1, 0)
            complete(near_way, 1, 1)

        def scores_tile(h, n):
            q = qbuf[g * groups + h, pl.ds(q_start, chunk), :]
            k = kv[direction, g, 0, pl.ds(k_start + n * KEY_TILE, KEY_TILE), :]
            s = lax.dot_general(q, k, (((1,), (1,)), ((), ())), preferred_element_type=jnp.float32)
            s = s * factor + bias[turn, :, n * KEY_TILE : (n + 1) * KEY_TILE]
            scores[h % 2, :, n * KEY_TILE : (n + 1) * KEY_TILE] = s
            return jnp.maximum(s[:, :HEAD], s[:, HEAD:])

        def value_tile(h, n, top):
            p = jnp.exp2(scores[h % 2, :, n * KEY_TILE : (n + 1) * KEY_TILE] - top)
            v = kv[direction, g, 1, pl.ds(k_start + n * KEY_TILE, KEY_TILE), :]
            product = jnp.dot(p.astype(jnp.bfloat16), v, preferred_element_type=jnp.float32)
            return product, p[:, :HEAD] + p[:, HEAD:]

        highest = scores_tile(0, 0)
        for n in range(1, key_tiles):
            highest = jnp.maximum(highest, scores_tile(0, n))

        @pl.when(u == 0)
        def _():
            complete(far_way, 0, 1)

        @pl.when(u > 0)
        def _():
            last_turn, last_g = place(u - 1)
            ship(last_turn, last_g * groups + groups - 1)

        for h in range(groups):
            top = jnp.max(highest, axis=1, keepdims=True)
            total = weight = highest = None
            for n in range(key_tiles):
                if h + 1 < groups:
                    tile = scores_tile(h + 1, n)
                    highest = tile if highest is None else jnp.maximum(highest, tile)
                product, part = value_tile(h, n, top)
                total = product if total is None else total + product
                weight = part if weight is None else weight + part
            weight = jnp.sum(weight, axis=1, keepdims=True)
            outs[turn, g * groups + h] = (total / weight).astype(outs.dtype)
            if h > 0:
                ship(turn, g * groups + h - 1)
        return carry

    lax.fori_loop(0, 4 * kv_local, unit, 0)

    keep(heads - 1).start()

    for g in range(kv_local):
        for part in range(2):
            for way in (far_way, near_way):
                @pl.when(hops(way))
                def _():
                    hop(way, g, part, 0).wait_send()

                @pl.when(detours(way))
                def _():
                    detour(g, part).wait_send()

                across(way, g, part, 0).wait_send()
                across(way, g, part, 1).wait_send()

                @pl.when(jnp.logical_not(stops(way)))
                def _():
                    hop(way, g, part, 1).wait_send()

                @pl.when(leaps(way))
                def _():
                    leap(way, g, part).wait_send()

    @pl.when(is_relay)
    def _():
        for g in range(kv_local):
            for part in range(2):
                forward(g, part).wait_send()

    def drain(i, carry):
        turn, h = i // heads, i % heads
        send(turn, h).wait_send()
        received(turn, h).wait_recv()
        return carry

    lax.fori_loop(0, 3 * heads, drain, 0)
    for h in range(heads):
        keep(h).wait()


def on_device(cp_size, tp_size, queries, keys, values, doc_lengths):
    tok_rows, q_cols = queries.shape
    half = tok_rows // 2
    kv_local = keys.shape[1] // HEAD
    heads = q_cols // HEAD
    groups = heads // kv_local
    chunk = tok_rows // tp_size
    window = 7 * KEY_TILE
    hbm = pl.BlockSpec(memory_space=pl.ANY)
    return pl.pallas_call(
        functools.partial(kernel, (cp_size, tp_size, half, groups, kv_local)),
        out_shape=pltpu.VMEM((chunk, q_cols * tp_size), jnp.bfloat16),
        in_specs=[pl.BlockSpec(memory_space=pltpu.VMEM), hbm, hbm, hbm],
        out_specs=pl.BlockSpec(memory_space=pltpu.VMEM),
        scratch_shapes=[
            pltpu.VMEM((2, kv_local, 2, 5 * half, HEAD), jnp.bfloat16),
            pltpu.VMEM((kv_local, 2, half, HEAD), jnp.bfloat16),
            pltpu.VMEM((heads, tok_rows, HEAD), jnp.bfloat16),
            pltpu.VMEM((4, chunk, window), jnp.float32),
            pltpu.VMEM((2, chunk, window), jnp.float32),
            pltpu.VMEM((4, heads, chunk, HEAD), jnp.bfloat16),
            pltpu.SemaphoreType.DMA((2, kv_local, 2)),
            pltpu.SemaphoreType.DMA((heads,)),
            pltpu.SemaphoreType.DMA((2, kv_local, 2, 4)),
            pltpu.SemaphoreType.DMA((2, kv_local, 2)),
            pltpu.SemaphoreType.DMA((2, kv_local, 2, 4)),
            pltpu.SemaphoreType.DMA((kv_local, 2)),
            pltpu.SemaphoreType.DMA((kv_local, 2)),
            pltpu.SemaphoreType.DMA((3, heads)),
            pltpu.SemaphoreType.DMA((3, heads)),
            pltpu.SemaphoreType.DMA((heads,)),
        ],
        compiler_params=pltpu.CompilerParams(
            collective_id=0, has_side_effects=True, vmem_limit_bytes=60 * 1024 * 1024
        ),
    )(doc_lengths, queries, keys, values)


def solution(mesh):
    in_specs = (P("cp", "tp"), P("cp", "tp"), P("cp", "tp"), P())
    out_specs = P(("cp", "tp"), None)
    return jax.shard_map(
        functools.partial(on_device, mesh.shape["cp"], mesh.shape["tp"]),
        mesh=mesh, in_specs=in_specs, out_specs=out_specs, check_vma=False,
    )
```

```python
import functools
import math

import jax
import jax.numpy as jnp
from jax import lax
from jax.experimental import pallas as pl
from jax.experimental.pallas import tpu as pltpu
from jax.sharding import PartitionSpec as P

HEAD = 128
MESH = pl.DeviceIdType.MESH
MASKED = -1e30
KEY_TILE = 256


def kernel(sizes, lens_ref, q_hbm, k_hbm, v_hbm, out_hbm, kv, passing, qbuf, bias, scores, outs,
           load_sem, q_sem, kv_send, leap_send, kv_recv, pass_send, pass_recv, out_send, out_recv, own_sem):
    cp_size, tp_size, half, groups, kv_local = sizes
    heads = groups * kv_local
    chunk = 2 * half // tp_size
    window = bias.shape[-1]
    key_tiles = window // KEY_TILE
    cp = lax.axis_index("cp")
    tp = lax.axis_index("tp")
    core = cp % 2
    partner = cp + 1 - 2 * core
    far_way = 1 - tp // 2
    near_way = tp // 2

    def slot(direction, g, part, which):
        return kv.at[direction, g, part, pl.ds(which * half, half), :]

    at_top = (cp >= cp_size - 2).astype(jnp.int32)
    at_bottom = (cp < 2).astype(jnp.int32)
    is_end = ((cp < 2) & (far_way == 0)) | ((cp >= cp_size - 2) & (far_way == 1))
    above = (1 - at_top) * (cp + 2) + at_top * partner
    below = (1 - at_bottom) * (cp - 2) + at_bottom * partner

    chips = cp_size // 2
    chip = cp // 2
    middle = chips // 2
    near_gap = (chip >= middle - 2) & (chip <= middle + 1)
    below_gap = (chip < middle).astype(jnp.int32)
    mate = cp - 4 + 8 * below_gap
    near_first = near_gap & (near_way == 1 - below_gap)

    along_x = math.isqrt(middle) - 1
    along_y = middle - math.isqrt(middle)
    odd = core == 1
    relays_up = odd & ((chip == middle - 1 - along_x) | (chip == middle - 2 - along_y))
    relays_down = odd & ((chip == middle + along_x) | (chip == middle + 1 + along_y))
    is_relay = relays_up | relays_down
    down = relays_down.astype(jnp.int32)
    for_slot_2 = ((chip == middle - 1 - along_x) | (chip == middle + along_x)).astype(jnp.int32)
    relay_slot = 2 * for_slot_2
    relay_target = 2 * (middle - down) + 1
    relay_source = cp + 2 * (for_slot_2 * along_x + (1 - for_slot_2) * along_y) * (1 - 2 * down)
    is_middle = (chip == middle - 1) | (chip == middle)
    at_middle = is_middle.astype(jnp.int32)
    detour_via = cp - 2 * (at_middle * along_x + (1 - at_middle) * along_y) * (2 * below_gap - 1)

    def beyond(direction):
        return (1 - direction) * above + direction * below

    def landing(direction):
        return (1 - direction) * at_top + direction * (1 - at_bottom)

    def lead(direction):
        return (1 - core) * (1 - direction) + core * direction

    def stops(direction):
        return chip == middle - 1 + direction

    def leaps(direction):
        return (chip == middle - 2 + 3 * direction) & (core == 0)

    def detours(direction):
        return odd & (stops(direction) | (chip == middle - 2 + 3 * direction))

    def hops(direction):
        return jnp.logical_not(odd & stops(direction))

    def load(direction, g, part):
        src = (k_hbm, v_hbm)[part]
        return pltpu.make_async_copy(
            src.at[pl.ds(pl.multiple_of(direction * half, half), half), pl.ds(g * HEAD, HEAD)],
            slot(direction, g, part, 4),
            load_sem.at[direction, g, part],
        )

    def load_q(h):
        return pltpu.make_async_copy(
            q_hbm.at[:, pl.ds(h * HEAD, HEAD)], qbuf.at[h], q_sem.at[h]
        )

    def hop(direction, g, part, far):
        return pltpu.make_async_remote_copy(
            src_ref=slot(direction, g, part, 4 - 2 * far),
            dst_ref=slot(landing(direction), g, part, 2 - 2 * far),
            send_sem=kv_send.at[direction, g, part, far],
            recv_sem=kv_recv.at[landing(direction), g, part, 2 - 2 * far],
            device_id=(beyond(direction), tp),
            device_id_type=MESH,
        )

    def leap(direction, g, part):
        return pltpu.make_async_remote_copy(
            src_ref=slot(direction, g, part, 4),
            dst_ref=slot(direction, g, part, 0),
            send_sem=leap_send.at[direction, g, part],
            recv_sem=kv_recv.at[direction, g, part, 0],
            device_id=(cp + 4 - 8 * direction, tp),
            device_id_type=MESH,
        )

    def detour(g, part):
        return pltpu.make_async_remote_copy(
            src_ref=slot(1 - below_gap, g, part, 4),
            dst_ref=passing.at[g, part],
            send_sem=leap_send.at[1 - below_gap, g, part],
            recv_sem=pass_recv.at[g, part],
            device_id=(detour_via, tp),
            device_id_type=MESH,
        )

    def forward(g, part):
        return pltpu.make_async_remote_copy(
            src_ref=passing.at[g, part],
            dst_ref=slot(down, g, part, relay_slot),
            send_sem=pass_send.at[g, part],
            recv_sem=kv_recv.at[down, g, part, relay_slot],
            device_id=(relay_target, tp),
            device_id_type=MESH,
        )

    def across(direction, g, part, far):
        return pltpu.make_async_remote_copy(
            src_ref=slot(direction, g, part, 2 * lead(direction) + 2 - 2 * far),
            dst_ref=slot(direction, g, part, 3 - 2 * far),
            send_sem=kv_send.at[direction, g, part, 2 + far],
            recv_sem=kv_recv.at[direction, g, part, 3 - 2 * far],
            device_id=(partner, tp),
            device_id_type=MESH,
        )

    def arrived(direction, g, part, which):
        pltpu.make_async_remote_copy(
            src_ref=slot(direction, g, part, which),
            dst_ref=slot(direction, g, part, which),
            send_sem=kv_send.at[direction, g, part, 0],
            recv_sem=kv_recv.at[direction, g, part, which],
            device_id=(partner, tp),
            device_id_type=MESH,
        ).wait_recv()

    def offer(direction, g, part):
        load(direction, g, part).wait()

        @pl.when(hops(direction))
        def _():
            hop(direction, g, part, 0).start()

        @pl.when(detours(direction))
        def _():
            detour(g, part).start()

        @pl.when(leaps(direction))
        def _():
            leap(direction, g, part).start()

        @pl.when(lead(direction) == 1)
        def _():
            across(direction, g, part, 0).start()

    def relay(direction, g, part):
        arrived(direction, g, part, 2)

        @pl.when(jnp.logical_not(stops(direction)))
        def _():
            hop(direction, g, part, 1).start()

        @pl.when(lead(direction) == 1)
        def _():
            across(direction, g, part, 1).start()

        @pl.when(lead(direction) == 0)
        def _():
            across(direction, g, part, 0).start()

    def complete(direction, g, part):
        arrived(direction, g, part, 0)

        @pl.when(lead(direction) == 0)
        def _():
            across(direction, g, part, 1).start()

        arrived(direction, g, part, 3)
        arrived(direction, g, part, 1)

    def peer_of(turn):
        n = 3 - turn
        high = (tp // 2 + n // 2) % 2
        low = (tp % 2 + n % 2 + n // 2) % 2
        return high, low

    def send(turn, h):
        high, low = peer_of(turn)
        return pltpu.make_async_remote_copy(
            src_ref=outs.at[turn, h],
            dst_ref=out_hbm.at[:, pl.ds((tp * heads + h) * HEAD, HEAD)],
            send_sem=out_send.at[turn, h],
            recv_sem=out_recv.at[turn, h],
            device_id=(cp, 2 * high + low),
            device_id_type=MESH,
        )

    def received(turn, h):
        high, low = peer_of(turn)
        return pltpu.make_async_remote_copy(
            src_ref=outs.at[turn, h],
            dst_ref=out_hbm.at[:, pl.ds(((2 * high + low) * heads + h) * HEAD, HEAD)],
            send_sem=out_send.at[turn, h],
            recv_sem=out_recv.at[turn, h],
            device_id=(cp, 2 * high + low),
            device_id_type=MESH,
        )

    def keep(h):
        return pltpu.make_async_copy(
            outs.at[3, h], out_hbm.at[:, pl.ds((tp * heads + h) * HEAD, HEAD)], own_sem.at[h]
        )

    barrier = pltpu.get_barrier_semaphore()
    for turn in range(3):
        high, low = peer_of(turn)
        pl.semaphore_signal(barrier, inc=1, device_id=(cp, 2 * high + low), device_id_type=MESH)
    pl.semaphore_signal(barrier, inc=1, device_id=(partner, tp), device_id_type=MESH)

    @pl.when(jnp.logical_not(odd & (chip == middle - 1)))
    def _():
        pl.semaphore_signal(barrier, inc=1, device_id=(above, tp), device_id_type=MESH)

    @pl.when(jnp.logical_not(odd & (chip == middle)))
    def _():
        pl.semaphore_signal(barrier, inc=1, device_id=(below, tp), device_id_type=MESH)

    @pl.when(is_middle & (core == 0))
    def _():
        pl.semaphore_signal(barrier, inc=1, device_id=(mate, tp), device_id_type=MESH)

    @pl.when(is_relay)
    def _():
        pl.semaphore_signal(barrier, inc=1, device_id=(relay_source, tp), device_id_type=MESH)

    @pl.when(is_middle & odd)
    def _():
        for step in (along_x, 1 + along_y):
            device = 2 * (below_gap * (middle + step) + (1 - below_gap) * (middle - 1 - step)) + 1
            pl.semaphore_signal(barrier, inc=1, device_id=(device, tp), device_id_type=MESH)

    for direction in (far_way, near_way):
        for g in range(kv_local):
            for part in range(2):
                load(direction, g, part).start()
    for h in range(heads):
        load_q(h).start()

    greetings = (
        6 + (near_gap & jnp.logical_not(is_middle)).astype(jnp.int32) + is_relay.astype(jnp.int32)
    )
    pl.semaphore_wait(barrier, greetings)

    offer(far_way, 0, 0)
    offer(far_way, 0, 1)

    @pl.when(jnp.logical_not(near_gap))
    def _():
        offer(near_way, 0, 0)
        offer(near_way, 0, 1)

    row = lax.broadcasted_iota(jnp.int32, (HEAD, HEAD), 0)
    col = lax.broadcasted_iota(jnp.int32, (HEAD, HEAD), 1)
    upper = (row <= col).astype(jnp.float32)
    docs = lens_ref.shape[-1]
    lens = jnp.concatenate(
        [lens_ref[...].reshape(1, docs).astype(jnp.float32), jnp.zeros((1, HEAD - docs), jnp.float32)], axis=1
    )
    lens = jnp.broadcast_to(lens, (8, HEAD))
    ends = jnp.dot(lens, upper, precision=lax.Precision.HIGHEST, preferred_element_type=jnp.float32)[:1]
    lens = lens[:1]
    for turn in range(4):
        high, low = peer_of(turn)
        block = high * (2 * cp_size - 1 - 2 * cp) + cp
        q_pos = (
            lax.broadcasted_iota(jnp.int32, (chunk, 1), 0) + (block * half + low * chunk)
        ).astype(jnp.float32)
        start = jnp.sum(jnp.where(ends <= q_pos, lens, 0.0), axis=1, keepdims=True)
        for n in range(key_tiles):
            k_pos = (
                lax.broadcasted_iota(jnp.int32, (1, KEY_TILE), 1)
                + ((block - 4) * half + low * HEAD + n * KEY_TILE)
            ).astype(jnp.float32)
            allowed = (k_pos >= start) & (k_pos <= q_pos)
            bias[turn, :, n * KEY_TILE : (n + 1) * KEY_TILE] = jnp.where(allowed, 0.0, MASKED)

    for h in range(heads):
        load_q(h).wait()

    @pl.when(near_gap)
    def _():
        for way, g in ((far_way, 1), (near_way, 0), (near_way, 1)):
            offer(way, g, 0)
            offer(way, g, 1)

    def pass_on(g):
        @pl.when(is_relay)
        def _():
            for part in range(2):
                pltpu.make_async_remote_copy(
                    src_ref=passing.at[g, part],
                    dst_ref=passing.at[g, part],
                    send_sem=pass_send.at[g, part],
                    recv_sem=pass_recv.at[g, part],
                    device_id=(relay_source, tp),
                    device_id_type=MESH,
                ).wait_recv()
                forward(g, part).start()

    pass_on(0)
    relay(far_way, 0, 0)
    relay(far_way, 0, 1)

    @pl.when(near_first)
    def _():
        relay(near_way, 0, 0)
        relay(near_way, 0, 1)

    @pl.when(jnp.logical_not(near_gap))
    def _():
        for way in (far_way, near_way):
            offer(way, 1, 0)
            offer(way, 1, 1)

    pass_on(1)

    @pl.when(is_end)
    def _():
        relay(near_way, 0, 0)
        relay(near_way, 0, 1)

    complete(far_way, 0, 0)

    factor = math.log2(math.e) / math.sqrt(HEAD)

    def ship(turn, h):
        @pl.when(turn < 3)
        def _():
            send(turn, h).start()

        @pl.when(turn == 3)
        def _():
            keep(h).start()

    def place(u):
        return 2 * (u // 4) + u % 2, (u // 2) % 2

    def unit(u, carry):
        turn, g = place(u)
        direction, low = peer_of(turn)
        q_start = pl.multiple_of(direction * half + low * chunk, 64)
        k_start = pl.multiple_of(low * HEAD, HEAD)

        @pl.when(u == 1)
        def _():
            relay(far_way, 1, 0)
            relay(far_way, 1, 1)

            @pl.when(near_first)
            def _():
                relay(near_way, 1, 0)
                relay(near_way, 1, 1)

        @pl.when(u == 2)
        def _():
            @pl.when(is_end)
            def _():
                relay(near_way, 1, 0)
                relay(near_way, 1, 1)

            complete(far_way, 1, 0)
            complete(far_way, 1, 1)

            @pl.when(jnp.logical_not(is_end | near_first))
            def _():
                relay(near_way, 0, 0)
                relay(near_way, 0, 1)

        @pl.when((u == 3) & jnp.logical_not(is_end | near_first))
        def _():
            relay(near_way, 1, 0)
            relay(near_way, 1, 1)

        @pl.when(u == 4)
        def _():
            complete(near_way, 0, 0)
            complete(near_way, 0, 1)

        @pl.when(u == 6)
        def _():
            complete(near_way, 1, 0)
            complete(near_way, 1, 1)

        def scores_tile(h, n):
            q = qbuf[g * groups + h, pl.ds(q_start, chunk), :]
            k = kv[direction, g, 0, pl.ds(k_start + n * KEY_TILE, KEY_TILE), :]
            s = lax.dot_general(q, k, (((1,), (1,)), ((), ())), preferred_element_type=jnp.float32)
            s = s * factor + bias[turn, :, n * KEY_TILE : (n + 1) * KEY_TILE]
            scores[h % 2, :, n * KEY_TILE : (n + 1) * KEY_TILE] = s
            return jnp.maximum(s[:, :HEAD], s[:, HEAD:])

        def value_tile(h, n, top):
            p = jnp.exp2(scores[h % 2, :, n * KEY_TILE : (n + 1) * KEY_TILE] - top)
            v = kv[direction, g, 1, pl.ds(k_start + n * KEY_TILE, KEY_TILE), :]
            product = jnp.dot(p.astype(jnp.bfloat16), v, preferred_element_type=jnp.float32)
            return product, p[:, :HEAD] + p[:, HEAD:]

        highest = scores_tile(0, 0)
        for n in range(1, key_tiles):
            highest = jnp.maximum(highest, scores_tile(0, n))

        @pl.when(u == 0)
        def _():
            complete(far_way, 0, 1)

        @pl.when(u > 0)
        def _():
            last_turn, last_g = place(u - 1)
            ship(last_turn, last_g * groups + groups - 1)

        for h in range(groups):
            top = jnp.max(highest, axis=1, keepdims=True)
            total = weight = highest = None
            for n in range(key_tiles):
                if h + 1 < groups:
                    tile = scores_tile(h + 1, n)
                    highest = tile if highest is None else jnp.maximum(highest, tile)
                product, part = value_tile(h, n, top)
                total = product if total is None else total + product
                weight = part if weight is None else weight + part
            weight = jnp.sum(weight, axis=1, keepdims=True)
            outs[turn, g * groups + h] = (total / weight).astype(outs.dtype)
            if h > 0:
                ship(turn, g * groups + h - 1)
        return carry

    lax.fori_loop(0, 4 * kv_local, unit, 0)

    keep(heads - 1).start()

    for g in range(kv_local):
        for part in range(2):
            for way in (far_way, near_way):
                @pl.when(hops(way))
                def _():
                    hop(way, g, part, 0).wait_send()

                @pl.when(detours(way))
                def _():
                    detour(g, part).wait_send()

                across(way, g, part, 0).wait_send()
                across(way, g, part, 1).wait_send()

                @pl.when(jnp.logical_not(stops(way)))
                def _():
                    hop(way, g, part, 1).wait_send()

                @pl.when(leaps(way))
                def _():
                    leap(way, g, part).wait_send()

    @pl.when(is_relay)
    def _():
        for g in range(kv_local):
            for part in range(2):
                forward(g, part).wait_send()

    def drain(i, carry):
        turn, h = i // heads, i % heads
        send(turn, h).wait_send()
        received(turn, h).wait_recv()
        return carry

    lax.fori_loop(0, 3 * heads, drain, 0)
    for h in range(heads):
        keep(h).wait()


def on_device(cp_size, tp_size, queries, keys, values, doc_lengths):
    tok_rows, q_cols = queries.shape
    half = tok_rows // 2
    kv_local = keys.shape[1] // HEAD
    heads = q_cols // HEAD
    groups = heads // kv_local
    chunk = tok_rows // tp_size
    window = 7 * KEY_TILE
    hbm = pl.BlockSpec(memory_space=pl.ANY)
    return pl.pallas_call(
        functools.partial(kernel, (cp_size, tp_size, half, groups, kv_local)),
        out_shape=pltpu.VMEM((chunk, q_cols * tp_size), jnp.bfloat16),
        in_specs=[pl.BlockSpec(memory_space=pltpu.VMEM), hbm, hbm, hbm],
        out_specs=pl.BlockSpec(memory_space=pltpu.VMEM),
        scratch_shapes=[
            pltpu.VMEM((2, kv_local, 2, 5 * half, HEAD), jnp.bfloat16),
            pltpu.VMEM((kv_local, 2, half, HEAD), jnp.bfloat16),
            pltpu.VMEM((heads, tok_rows, HEAD), jnp.bfloat16),
            pltpu.VMEM((4, chunk, window), jnp.float32),
            pltpu.VMEM((2, chunk, window), jnp.float32),
            pltpu.VMEM((4, heads, chunk, HEAD), jnp.bfloat16),
            pltpu.SemaphoreType.DMA((2, kv_local, 2)),
            pltpu.SemaphoreType.DMA((heads,)),
            pltpu.SemaphoreType.DMA((2, kv_local, 2, 4)),
            pltpu.SemaphoreType.DMA((2, kv_local, 2)),
            pltpu.SemaphoreType.DMA((2, kv_local, 2, 4)),
            pltpu.SemaphoreType.DMA((kv_local, 2)),
            pltpu.SemaphoreType.DMA((kv_local, 2)),
            pltpu.SemaphoreType.DMA((3, heads)),
            pltpu.SemaphoreType.DMA((3, heads)),
            pltpu.SemaphoreType.DMA((heads,)),
        ],
        compiler_params=pltpu.CompilerParams(
            collective_id=0, has_side_effects=True, vmem_limit_bytes=60 * 1024 * 1024
        ),
    )(doc_lengths, queries, keys, values)


def solution(mesh):
    in_specs = (P("cp", "tp"), P("cp", "tp"), P("cp", "tp"), P())
    out_specs = P(("cp", "tp"), None)
    return jax.shard_map(
        functools.partial(on_device, mesh.shape["cp"], mesh.shape["tp"]),
        mesh=mesh, in_specs=in_specs, out_specs=out_specs, check_vma=False,
    )
```

```python
import functools
import math

import jax
import jax.numpy as jnp
from jax import lax
from jax.experimental import pallas as pl
from jax.experimental.pallas import tpu as pltpu
from jax.sharding import PartitionSpec as P

HEAD = 128
MESH = pl.DeviceIdType.MESH
MASKED = -1e30
KEY_TILE = 256


def kernel(sizes, lens_hbm, q_hbm, k_hbm, v_hbm, out_hbm, kv, passing, qbuf, bias, scores, outs,
           load_sem, q_sem, kv_send, leap_send, kv_recv, pass_send, pass_recv, out_send, out_recv, own_sem,
           lens_ref, lens_sem):
    cp_size, tp_size, half, groups, kv_local = sizes
    heads = groups * kv_local
    chunk = 2 * half // tp_size
    window = bias.shape[-1]
    key_tiles = window // KEY_TILE
    cp = lax.axis_index("cp")
    tp = lax.axis_index("tp")
    core = cp % 2
    partner = cp + 1 - 2 * core
    far_way = 1 - tp // 2
    near_way = tp // 2

    def slot(direction, g, part, which):
        return kv.at[direction, g, part, pl.ds(which * half, half), :]

    at_top = (cp >= cp_size - 2).astype(jnp.int32)
    at_bottom = (cp < 2).astype(jnp.int32)
    is_end = ((cp < 2) & (far_way == 0)) | ((cp >= cp_size - 2) & (far_way == 1))
    above = (1 - at_top) * (cp + 2) + at_top * partner
    below = (1 - at_bottom) * (cp - 2) + at_bottom * partner

    chips = cp_size // 2
    chip = cp // 2
    middle = chips // 2
    near_gap = (chip >= middle - 2) & (chip <= middle + 1)
    below_gap = (chip < middle).astype(jnp.int32)
    mate = cp - 4 + 8 * below_gap
    near_first = near_gap & (near_way == 1 - below_gap)

    along_x = math.isqrt(middle) - 1
    along_y = middle - math.isqrt(middle)
    odd = core == 1
    relays_up = odd & ((chip == middle - 1 - along_x) | (chip == middle - 2 - along_y))
    relays_down = odd & ((chip == middle + along_x) | (chip == middle + 1 + along_y))
    is_relay = relays_up | relays_down
    down = relays_down.astype(jnp.int32)
    for_slot_2 = ((chip == middle - 1 - along_x) | (chip == middle + along_x)).astype(jnp.int32)
    relay_slot = 2 * for_slot_2
    relay_target = 2 * (middle - down) + 1
    relay_source = cp + 2 * (for_slot_2 * along_x + (1 - for_slot_2) * along_y) * (1 - 2 * down)
    is_middle = (chip == middle - 1) | (chip == middle)
    at_middle = is_middle.astype(jnp.int32)
    detour_via = cp - 2 * (at_middle * along_x + (1 - at_middle) * along_y) * (2 * below_gap - 1)

    def beyond(direction):
        return (1 - direction) * above + direction * below

    def landing(direction):
        return (1 - direction) * at_top + direction * (1 - at_bottom)

    def lead(direction):
        return (1 - core) * (1 - direction) + core * direction

    def stops(direction):
        return chip == middle - 1 + direction

    def leaps(direction):
        return (chip == middle - 2 + 3 * direction) & (core == 0)

    def detours(direction):
        return odd & (stops(direction) | (chip == middle - 2 + 3 * direction))

    def hops(direction):
        return jnp.logical_not(odd & stops(direction))

    def load(direction, g, part):
        src = (k_hbm, v_hbm)[part]
        return pltpu.make_async_copy(
            src.at[pl.ds(pl.multiple_of(direction * half, half), half), pl.ds(g * HEAD, HEAD)],
            slot(direction, g, part, 4),
            load_sem.at[direction, g, part],
        )

    def load_q(h):
        return pltpu.make_async_copy(
            q_hbm.at[:, pl.ds(h * HEAD, HEAD)], qbuf.at[h], q_sem.at[h]
        )

    def hop(direction, g, part, far):
        return pltpu.make_async_remote_copy(
            src_ref=slot(direction, g, part, 4 - 2 * far),
            dst_ref=slot(landing(direction), g, part, 2 - 2 * far),
            send_sem=kv_send.at[direction, g, part, far],
            recv_sem=kv_recv.at[landing(direction), g, part, 2 - 2 * far],
            device_id=(beyond(direction), tp),
            device_id_type=MESH,
        )

    def leap(direction, g, part):
        return pltpu.make_async_remote_copy(
            src_ref=slot(direction, g, part, 4),
            dst_ref=slot(direction, g, part, 0),
            send_sem=leap_send.at[direction, g, part],
            recv_sem=kv_recv.at[direction, g, part, 0],
            device_id=(cp + 4 - 8 * direction, tp),
            device_id_type=MESH,
        )

    def detour(g, part):
        return pltpu.make_async_remote_copy(
            src_ref=slot(1 - below_gap, g, part, 4),
            dst_ref=passing.at[g, part],
            send_sem=leap_send.at[1 - below_gap, g, part],
            recv_sem=pass_recv.at[g, part],
            device_id=(detour_via, tp),
            device_id_type=MESH,
        )

    def forward(g, part):
        return pltpu.make_async_remote_copy(
            src_ref=passing.at[g, part],
            dst_ref=slot(down, g, part, relay_slot),
            send_sem=pass_send.at[g, part],
            recv_sem=kv_recv.at[down, g, part, relay_slot],
            device_id=(relay_target, tp),
            device_id_type=MESH,
        )

    def across(direction, g, part, far):
        return pltpu.make_async_remote_copy(
            src_ref=slot(direction, g, part, 2 * lead(direction) + 2 - 2 * far),
            dst_ref=slot(direction, g, part, 3 - 2 * far),
            send_sem=kv_send.at[direction, g, part, 2 + far],
            recv_sem=kv_recv.at[direction, g, part, 3 - 2 * far],
            device_id=(partner, tp),
            device_id_type=MESH,
        )

    def arrived(direction, g, part, which):
        pltpu.make_async_remote_copy(
            src_ref=slot(direction, g, part, which),
            dst_ref=slot(direction, g, part, which),
            send_sem=kv_send.at[direction, g, part, 0],
            recv_sem=kv_recv.at[direction, g, part, which],
            device_id=(partner, tp),
            device_id_type=MESH,
        ).wait_recv()

    def offer(direction, g, part):
        load(direction, g, part).wait()

        @pl.when(hops(direction))
        def _():
            hop(direction, g, part, 0).start()

        @pl.when(detours(direction))
        def _():
            detour(g, part).start()

        @pl.when(leaps(direction))
        def _():
            leap(direction, g, part).start()

        @pl.when(lead(direction) == 1)
        def _():
            across(direction, g, part, 0).start()

    def relay(direction, g, part):
        arrived(direction, g, part, 2)

        @pl.when(jnp.logical_not(stops(direction)))
        def _():
            hop(direction, g, part, 1).start()

        @pl.when(lead(direction) == 1)
        def _():
            across(direction, g, part, 1).start()

        @pl.when(lead(direction) == 0)
        def _():
            across(direction, g, part, 0).start()

    def complete(direction, g, part):
        arrived(direction, g, part, 0)

        @pl.when(lead(direction) == 0)
        def _():
            across(direction, g, part, 1).start()

        arrived(direction, g, part, 3)
        arrived(direction, g, part, 1)

    def peer_of(turn):
        n = 3 - turn
        high = (tp // 2 + n // 2) % 2
        low = (tp % 2 + n % 2 + n // 2) % 2
        return high, low

    def send(turn, h):
        high, low = peer_of(turn)
        return pltpu.make_async_remote_copy(
            src_ref=outs.at[turn, h],
            dst_ref=out_hbm.at[:, pl.ds((tp * heads + h) * HEAD, HEAD)],
            send_sem=out_send.at[turn, h],
            recv_sem=out_recv.at[turn, h],
            device_id=(cp, 2 * high + low),
            device_id_type=MESH,
        )

    def received(turn, h):
        high, low = peer_of(turn)
        return pltpu.make_async_remote_copy(
            src_ref=outs.at[turn, h],
            dst_ref=out_hbm.at[:, pl.ds(((2 * high + low) * heads + h) * HEAD, HEAD)],
            send_sem=out_send.at[turn, h],
            recv_sem=out_recv.at[turn, h],
            device_id=(cp, 2 * high + low),
            device_id_type=MESH,
        )

    def keep(h):
        return pltpu.make_async_copy(
            outs.at[3, h], out_hbm.at[:, pl.ds((tp * heads + h) * HEAD, HEAD)], own_sem.at[h]
        )

    barrier = pltpu.get_barrier_semaphore()
    for turn in range(3):
        high, low = peer_of(turn)
        pl.semaphore_signal(barrier, inc=1, device_id=(cp, 2 * high + low), device_id_type=MESH)
    pl.semaphore_signal(barrier, inc=1, device_id=(partner, tp), device_id_type=MESH)

    @pl.when(jnp.logical_not(odd & (chip == middle - 1)))
    def _():
        pl.semaphore_signal(barrier, inc=1, device_id=(above, tp), device_id_type=MESH)

    @pl.when(jnp.logical_not(odd & (chip == middle)))
    def _():
        pl.semaphore_signal(barrier, inc=1, device_id=(below, tp), device_id_type=MESH)

    @pl.when(is_middle & (core == 0))
    def _():
        pl.semaphore_signal(barrier, inc=1, device_id=(mate, tp), device_id_type=MESH)

    @pl.when(is_relay)
    def _():
        pl.semaphore_signal(barrier, inc=1, device_id=(relay_source, tp), device_id_type=MESH)

    @pl.when(is_middle & odd)
    def _():
        for step in (along_x, 1 + along_y):
            device = 2 * (below_gap * (middle + step) + (1 - below_gap) * (middle - 1 - step)) + 1
            pl.semaphore_signal(barrier, inc=1, device_id=(device, tp), device_id_type=MESH)

    for direction in (far_way, near_way):
        for g in range(kv_local):
            for part in range(2):
                load(direction, g, part).start()
    load_lens = pltpu.make_async_copy(lens_hbm, lens_ref, lens_sem)
    load_lens.start()
    for h in range(heads):
        load_q(h).start()

    greetings = (
        6 + (near_gap & jnp.logical_not(is_middle)).astype(jnp.int32) + is_relay.astype(jnp.int32)
    )
    pl.semaphore_wait(barrier, greetings)

    offer(far_way, 0, 0)
    offer(far_way, 0, 1)

    @pl.when(jnp.logical_not(near_gap))
    def _():
        offer(near_way, 0, 0)
        offer(near_way, 0, 1)

    row = lax.broadcasted_iota(jnp.int32, (HEAD, HEAD), 0)
    col = lax.broadcasted_iota(jnp.int32, (HEAD, HEAD), 1)
    upper = (row <= col).astype(jnp.float32)
    load_lens.wait()
    docs = lens_ref.shape[-1]
    lens = jnp.concatenate(
        [lens_ref[...].reshape(1, docs).astype(jnp.float32), jnp.zeros((1, HEAD - docs), jnp.float32)], axis=1
    )
    lens = jnp.broadcast_to(lens, (8, HEAD))
    ends = jnp.dot(lens, upper, precision=lax.Precision.HIGHEST, preferred_element_type=jnp.float32)[:1]
    lens = lens[:1]
    for turn in range(4):
        high, low = peer_of(turn)
        block = high * (2 * cp_size - 1 - 2 * cp) + cp
        q_pos = (
            lax.broadcasted_iota(jnp.int32, (chunk, 1), 0) + (block * half + low * chunk)
        ).astype(jnp.float32)
        start = jnp.sum(jnp.where(ends <= q_pos, lens, 0.0), axis=1, keepdims=True)
        for n in range(key_tiles):
            k_pos = (
                lax.broadcasted_iota(jnp.int32, (1, KEY_TILE), 1)
                + ((block - 4) * half + low * HEAD + n * KEY_TILE)
            ).astype(jnp.float32)
            allowed = (k_pos >= start) & (k_pos <= q_pos)
            bias[turn, :, n * KEY_TILE : (n + 1) * KEY_TILE] = jnp.where(allowed, 0.0, MASKED)

    for h in range(heads):
        load_q(h).wait()

    @pl.when(near_gap)
    def _():
        for way, g in ((far_way, 1), (near_way, 0), (near_way, 1)):
            offer(way, g, 0)
            offer(way, g, 1)

    def pass_on(g):
        @pl.when(is_relay)
        def _():
            for part in range(2):
                pltpu.make_async_remote_copy(
                    src_ref=passing.at[g, part],
                    dst_ref=passing.at[g, part],
                    send_sem=pass_send.at[g, part],
                    recv_sem=pass_recv.at[g, part],
                    device_id=(relay_source, tp),
                    device_id_type=MESH,
                ).wait_recv()
                forward(g, part).start()

    pass_on(0)
    relay(far_way, 0, 0)
    relay(far_way, 0, 1)

    @pl.when(near_first)
    def _():
        relay(near_way, 0, 0)
        relay(near_way, 0, 1)

    @pl.when(jnp.logical_not(near_gap))
    def _():
        for way in (far_way, near_way):
            offer(way, 1, 0)
            offer(way, 1, 1)

    pass_on(1)

    @pl.when(is_end)
    def _():
        relay(near_way, 0, 0)
        relay(near_way, 0, 1)

    complete(far_way, 0, 0)

    factor = math.log2(math.e) / math.sqrt(HEAD)

    def ship(turn, h):
        @pl.when(turn < 3)
        def _():
            send(turn, h).start()

        @pl.when(turn == 3)
        def _():
            keep(h).start()

    def place(u):
        return 2 * (u // 4) + u % 2, (u // 2) % 2

    def unit(u, carry):
        turn, g = place(u)
        direction, low = peer_of(turn)
        q_start = pl.multiple_of(direction * half + low * chunk, 64)
        k_start = pl.multiple_of(low * HEAD, HEAD)

        @pl.when(u == 1)
        def _():
            relay(far_way, 1, 0)
            relay(far_way, 1, 1)

            @pl.when(near_first)
            def _():
                relay(near_way, 1, 0)
                relay(near_way, 1, 1)

        @pl.when(u == 2)
        def _():
            @pl.when(is_end)
            def _():
                relay(near_way, 1, 0)
                relay(near_way, 1, 1)

            complete(far_way, 1, 0)
            complete(far_way, 1, 1)

            @pl.when(jnp.logical_not(is_end | near_first))
            def _():
                relay(near_way, 0, 0)
                relay(near_way, 0, 1)

        @pl.when((u == 3) & jnp.logical_not(is_end | near_first))
        def _():
            relay(near_way, 1, 0)
            relay(near_way, 1, 1)

        @pl.when(u == 4)
        def _():
            complete(near_way, 0, 0)
            complete(near_way, 0, 1)

        @pl.when(u == 6)
        def _():
            complete(near_way, 1, 0)
            complete(near_way, 1, 1)

        def scores_tile(h, n):
            q = qbuf[g * groups + h, pl.ds(q_start, chunk), :]
            k = kv[direction, g, 0, pl.ds(k_start + n * KEY_TILE, KEY_TILE), :]
            s = lax.dot_general(q, k, (((1,), (1,)), ((), ())), preferred_element_type=jnp.float32)
            s = s * factor + bias[turn, :, n * KEY_TILE : (n + 1) * KEY_TILE]
            scores[h % 2, :, n * KEY_TILE : (n + 1) * KEY_TILE] = s
            return jnp.maximum(s[:, :HEAD], s[:, HEAD:])

        def value_tile(h, n, top):
            p = jnp.exp2(scores[h % 2, :, n * KEY_TILE : (n + 1) * KEY_TILE] - top)
            v = kv[direction, g, 1, pl.ds(k_start + n * KEY_TILE, KEY_TILE), :]
            product = jnp.dot(p.astype(jnp.bfloat16), v, preferred_element_type=jnp.float32)
            return product, p[:, :HEAD] + p[:, HEAD:]

        highest = scores_tile(0, 0)
        for n in range(1, key_tiles):
            highest = jnp.maximum(highest, scores_tile(0, n))

        @pl.when(u == 0)
        def _():
            complete(far_way, 0, 1)

        @pl.when(u > 0)
        def _():
            last_turn, last_g = place(u - 1)
            ship(last_turn, last_g * groups + groups - 1)

        for h in range(groups):
            top = jnp.max(highest, axis=1, keepdims=True)
            total = weight = highest = None
            for n in range(key_tiles):
                if h + 1 < groups:
                    tile = scores_tile(h + 1, n)
                    highest = tile if highest is None else jnp.maximum(highest, tile)
                product, part = value_tile(h, n, top)
                total = product if total is None else total + product
                weight = part if weight is None else weight + part
            weight = jnp.sum(weight, axis=1, keepdims=True)
            outs[turn, g * groups + h] = (total / weight).astype(outs.dtype)
            if h > 0:
                ship(turn, g * groups + h - 1)
        return carry

    lax.fori_loop(0, 4 * kv_local, unit, 0)

    keep(heads - 1).start()

    for g in range(kv_local):
        for part in range(2):
            for way in (far_way, near_way):
                @pl.when(hops(way))
                def _():
                    hop(way, g, part, 0).wait_send()

                @pl.when(detours(way))
                def _():
                    detour(g, part).wait_send()

                across(way, g, part, 0).wait_send()
                across(way, g, part, 1).wait_send()

                @pl.when(jnp.logical_not(stops(way)))
                def _():
                    hop(way, g, part, 1).wait_send()

                @pl.when(leaps(way))
                def _():
                    leap(way, g, part).wait_send()

    @pl.when(is_relay)
    def _():
        for g in range(kv_local):
            for part in range(2):
                forward(g, part).wait_send()

    def drain(i, carry):
        turn, h = i // heads, i % heads
        send(turn, h).wait_send()
        received(turn, h).wait_recv()
        return carry

    lax.fori_loop(0, 3 * heads, drain, 0)
    for h in range(heads):
        keep(h).wait()


def on_device(cp_size, tp_size, queries, keys, values, doc_lengths):
    tok_rows, q_cols = queries.shape
    half = tok_rows // 2
    kv_local = keys.shape[1] // HEAD
    heads = q_cols // HEAD
    groups = heads // kv_local
    chunk = tok_rows // tp_size
    window = 7 * KEY_TILE
    hbm = pl.BlockSpec(memory_space=pl.ANY)
    return pl.pallas_call(
        functools.partial(kernel, (cp_size, tp_size, half, groups, kv_local)),
        out_shape=pltpu.VMEM((chunk, q_cols * tp_size), jnp.bfloat16),
        in_specs=[hbm, hbm, hbm, hbm],
        out_specs=pl.BlockSpec(memory_space=pltpu.VMEM),
        scratch_shapes=[
            pltpu.VMEM((2, kv_local, 2, 5 * half, HEAD), jnp.bfloat16),
            pltpu.VMEM((kv_local, 2, half, HEAD), jnp.bfloat16),
            pltpu.VMEM((heads, tok_rows, HEAD), jnp.bfloat16),
            pltpu.VMEM((4, chunk, window), jnp.float32),
            pltpu.VMEM((2, chunk, window), jnp.float32),
            pltpu.VMEM((4, heads, chunk, HEAD), jnp.bfloat16),
            pltpu.SemaphoreType.DMA((2, kv_local, 2)),
            pltpu.SemaphoreType.DMA((heads,)),
            pltpu.SemaphoreType.DMA((2, kv_local, 2, 4)),
            pltpu.SemaphoreType.DMA((2, kv_local, 2)),
            pltpu.SemaphoreType.DMA((2, kv_local, 2, 4)),
            pltpu.SemaphoreType.DMA((kv_local, 2)),
            pltpu.SemaphoreType.DMA((kv_local, 2)),
            pltpu.SemaphoreType.DMA((3, heads)),
            pltpu.SemaphoreType.DMA((3, heads)),
            pltpu.SemaphoreType.DMA((heads,)),
            pltpu.VMEM(doc_lengths.shape, jnp.int32),
            pltpu.SemaphoreType.DMA,
        ],
        compiler_params=pltpu.CompilerParams(
            collective_id=0, has_side_effects=True, vmem_limit_bytes=60 * 1024 * 1024
        ),
    )(doc_lengths, queries, keys, values)


def solution(mesh):
    in_specs = (P("cp", "tp"), P("cp", "tp"), P("cp", "tp"), P())
    out_specs = P(("cp", "tp"), None)
    return jax.shard_map(
        functools.partial(on_device, mesh.shape["cp"], mesh.shape["tp"]),
        mesh=mesh, in_specs=in_specs, out_specs=out_specs, check_vma=False,
    )
```
